32 devices in a mesh: group: 4 (over z), batch: 8 (over y, x, core).
Axes of the slice: x: 2, y: 2, z: 4, core: 2. Of those that a mesh axis runs over, the one named last changes fastest.
Arguments:
- embeds: bfloat16 [65536, 256], P(('group', 'batch')), may hold values from -6 to 6
- out_grad: bfloat16 [65536, 256], P(('group', 'batch')), may hold values from -48 to 48
- w_query: bfloat16 [256, 256], replicated, may hold values from -0.375 to 0.375
- w_key: bfloat16 [256, 256], replicated, may hold values from -0.375 to 0.375
- w_value: bfloat16 [256, 256], replicated, may hold values from -0.375 to 0.375
- lengths: int32 [128], P(('group', 'batch')), may hold values from 1 to 512, as said below
- item_rows: int32 [65536], P(('group', 'batch')), may hold values from 0 to 2047, as said below
- tile_owner: int32 [512], P(('group', 'batch')), may hold values from 0 to 3, as said below
Outputs:
- table_grad: float32 [8192, 256], P(('group', 'batch'))
The draws below stay inside these ranges and needn't reach their ends.
Inputs may be any that keep to these rules, and one draw needn't show every extreme that they name: `lengths`: a history's live tokens are its first positions; in every draw some history has exactly 512 live tokens. `tile_owner`: among the first 8 tiles of each device's own tiles, and among the last 8, every group owns exactly 2 tiles. `item_rows`: of the 128 tokens of each tile, at most 32 have rows r with the same r // 256, and in every tile some value of r // 256 is taken by exactly 32 tokens.
All inputs are finite; a program needn't handle non-finite values.
Results may differ from the reference program's by a relative error of at most 0.0024.
The reference program's roundings to bfloat16 on the way (of `attend`, `value_grad`, `score_grad` and `token_grad`) count: a program that leaves them out, or rounds other values in their place, can miss the bound.
Values may be sent and summed in bfloat16 or wider, within the bound.
No kernel may reach another device: no remote copies, remote signals or barrier semaphores. Data moves between devices by JAX's collectives and lax.ppermute only.
A program may use at most 64 MiB of HBM per device.

```python
import math
import jax
import jax.numpy as jnp
from jax import lax

D = 256
HEADS = 2
DH = 128
TILE = 128
SEQ_LEN = 512
SEQ_DEV = 4
ROWS_DEV = 256
GROUPS = 4
BATCHES = 8
TILE_MOST = 32
ROWS_GRP = 2048
ITEMS = 8192
SEQS = 128
TOKENS = 65536
TILES_DEV = 16
TILES = 512


def draw_lengths(key, part):
    stream = jax.random.fold_in(key, 11)
    index = jnp.arange(SEQS, dtype=jnp.int32)
    device = index // SEQ_DEV
    column = device % BATCHES
    upper = SEQ_LEN * (BATCHES - 1 + 2 * column) // (3 * (BATCHES - 1))
    lower = jnp.maximum(upper // 2, 1)
    drawn = jax.random.randint(stream, (SEQS,), lower, upper + 1)
    longest = (column == BATCHES - 1) & (index % SEQ_DEV == SEQ_DEV - 1)
    return jnp.where(longest, SEQ_LEN, drawn).astype(jnp.int32)


def draw_tile_owner(key, part):
    stream = jax.random.fold_in(key, 23)
    half_tiles = TILES_DEV // 2
    block_count = TILES // half_tiles
    raw_scores = jax.random.randint(stream, (block_count, half_tiles), 0, 1 << 20)
    scores = raw_scores * half_tiles + jnp.arange(half_tiles, dtype=jnp.int32)[None, :]
    ranking = jnp.argsort(jnp.argsort(scores, axis=1), axis=1)
    return (ranking % GROUPS).reshape(TILES).astype(jnp.int32)


def draw_item_rows(key, part):
    owners = draw_tile_owner(key, part)
    tile_index = jnp.arange(TILES, dtype=jnp.int32)
    column = tile_index // TILES_DEV % BATCHES
    offsets = jax.random.randint(jax.random.fold_in(key, 31), (GROUPS,), 0, BATCHES)
    hottest = (column + offsets[owners]) % BATCHES
    pool_size = (BATCHES - 1) * TILE_MOST
    counter = jnp.arange(pool_size, dtype=jnp.int32)
    pool = (hottest[:, None] + 1 + counter[None, :] // TILE_MOST) % BATCHES
    pool_scores = jax.random.randint(jax.random.fold_in(key, 37), (TILES, pool_size), 0, 1 << 20) * pool_size + counter[None, :]
    pool_order = jnp.argsort(pool_scores, axis=1)
    picked = jnp.take_along_axis(pool, pool_order, axis=1)[:, :TILE - TILE_MOST]
    hot_block = jnp.broadcast_to(hottest[:, None], (TILES, TILE_MOST))
    joined = jnp.concatenate([hot_block, picked], axis=1)
    place_scores = jax.random.randint(jax.random.fold_in(key, 41), (TILES, TILE), 0, 1 << 20) * TILE + jnp.arange(TILE, dtype=jnp.int32)[None, :]
    place_order = jnp.argsort(place_scores, axis=1)
    holder = jnp.take_along_axis(joined, place_order, axis=1)
    drawn = jax.random.randint(jax.random.fold_in(key, 43), (TILES, TILE), 0, ROWS_DEV)
    local_row = drawn * drawn // ROWS_DEV
    return (holder * ROWS_DEV + local_row).reshape(TOKENS).astype(jnp.int32)


def levels(stream_key, dims, split, least, top_value):
    gain = 1.0
    for dim, shards_of in split:
        steps = jax.random.uniform(jax.random.fold_in(jax.random.fold_in(stream_key, 6), dim), (shards_of,), jnp.float32, least / len(split), top_value / len(split))
        gain = gain * jnp.repeat(jnp.exp(steps), dims[dim] // shards_of).reshape((-1,) + (1,) * (len(dims) - 1 - dim))
    return gain


def scatter_about(own_key, extent, spread, most, cuts=(), kind=jnp.bfloat16):
    loudness = levels(own_key, extent, cuts, -0.22, 0.18) if cuts else 1.0
    values = jax.random.normal(own_key, extent, jnp.float32) * spread * loudness
    return jnp.minimum(jnp.maximum(values, -most), most).astype(kind)


def setup_inputs(seed: int = 0) -> dict:
    splits = jax.random.split(jax.random.key(seed), 9)
    return {
        "embeds": scatter_about(splits[0], (TOKENS, D), 1.0, 6.0, ((0, 32),)),
        "out_grad": scatter_about(splits[1], (TOKENS, D), 8.0, 48.0, ((0, 32),)),
        "w_query": scatter_about(splits[2], (D, D), D ** -0.5, 0.375),
        "w_key": scatter_about(splits[3], (D, D), D ** -0.5, 0.375),
        "w_value": scatter_about(splits[4], (D, D), D ** -0.5, 0.375),
        "lengths": draw_lengths(jax.random.fold_in(splits[8], 71), 0),
        "item_rows": draw_item_rows(jax.random.fold_in(splits[8], 71), 0),
        "tile_owner": draw_tile_owner(jax.random.fold_in(splits[8], 71), 0),
    }


def sequence_grads(query, key_rows, value, grad_out, count, w_query, w_key, w_value):
    span = query.shape[0]
    position = lax.broadcasted_iota(jnp.int32, (span, span), 0)
    other = lax.broadcasted_iota(jnp.int32, (span, span), 1)
    live = ((other <= position) & (position < count)).astype(jnp.float32)
    weight = live / count.astype(jnp.float32)
    scale = 1.0 / math.sqrt(query.shape[2])
    highest = lax.Precision.HIGHEST
    query_f = query.astype(jnp.float32)
    key_f = key_rows.astype(jnp.float32)
    value_f = value.astype(jnp.float32)
    grad_f = grad_out.astype(jnp.float32)
    scores = jnp.einsum('ihd,jhd->hij', query_f, key_f, precision=highest) * scale
    sigma = jax.nn.sigmoid(scores)
    attend = (scores * sigma * weight).astype(jnp.bfloat16)
    value_grad = jnp.einsum('hij,ihd->jhd', attend.astype(jnp.float32), grad_f, precision=highest).astype(jnp.bfloat16)
    attend_grad = jnp.einsum('ihd,jhd->hij', grad_f, value_f, precision=highest)
    score_grad = (attend_grad * weight * sigma * (1.0 + scores * (1.0 - sigma))).astype(jnp.bfloat16)
    score_f = score_grad.astype(jnp.float32)
    query_grad = (jnp.einsum('hij,jhd->ihd', score_f, key_f, precision=highest) * scale).astype(jnp.bfloat16)
    key_grad = (jnp.einsum('hij,ihd->jhd', score_f, query_f, precision=highest) * scale).astype(jnp.bfloat16)
    width = w_query.shape[0]
    token = jnp.dot(query_grad.reshape(span, width), w_query.T, preferred_element_type=jnp.float32)
    token = token + jnp.dot(key_grad.reshape(span, width), w_key.T, preferred_element_type=jnp.float32)
    token = token + jnp.dot(value_grad.reshape(span, width), w_value.T, preferred_element_type=jnp.float32)
    return token.astype(jnp.bfloat16)

def reference(embeds, out_grad, w_query, w_key, w_value, lengths, item_rows, tile_owner):

    def project(weight_matrix):
        return jnp.dot(embeds, weight_matrix, preferred_element_type=jnp.float32).astype(jnp.bfloat16).reshape(SEQS, SEQ_LEN, HEADS, DH)
    query = project(w_query)
    key_rows = project(w_key)
    value = project(w_value)
    grad_heads = out_grad.reshape(SEQS, SEQ_LEN, HEADS, DH)

    def one_history(item):
        return sequence_grads(item[0], item[1], item[2], item[3], item[4], w_query, w_key, w_value)
    token_grad = lax.map(one_history, (query, key_rows, value, grad_heads, lengths)).reshape(TOKENS, D)
    table_rows = (jnp.repeat(tile_owner, TILE) * ROWS_GRP + item_rows).astype(jnp.int32)
    summed = jax.ops.segment_sum(token_grad.astype(jnp.float32), table_rows, num_segments=ITEMS)
    live_total = jnp.sum(lengths.astype(jnp.float32))
    return TOKENS / live_total * summed
```

```python
import functools
import math

import jax
import jax.numpy as jnp
from jax import lax
from jax.experimental import pallas as pl
from jax.experimental.pallas import tpu as pltpu
from jax.sharding import PartitionSpec as P

HEADS = 2
ROWS_DEV = 256
EXTRA = 16
BASE = 128
NT = (((1,), (1,)), ((), ()))
TN = (((0,), (0,)), ((), ()))


def dot(a, b, dims=(((1,), (0,)), ((), ()))):
    return lax.dot_general(a, b, dims, preferred_element_type=jnp.float32)


def digits_row(total, width):
    lane = lax.broadcasted_iota(jnp.int32, (1, width), 1)
    low, mid, high = total % BASE, (total // BASE) % BASE, total // (BASE * BASE)
    row = jnp.where(lane == 0, low, jnp.where(lane == 1, mid, jnp.where(lane == 2, high, 0)))
    return row.astype(jnp.float32)


def total_of_digits(row):
    return row[:, 0:1] + row[:, 1:2] * float(BASE) + row[:, 2:3] * float(BASE * BASE)


def attention_kernel(
    half, half_seqs, half_tiles, groups, tile, extra,
    len_ref, own_ref, emb, gout, wq, wk, wv, rows, *refs,
):
    outs = refs[:groups]
    q_s, k_s, v_s, dq_s, dk_s, dv_s, tok_s, ext_s, idx_s = refs[groups:]
    step = pl.program_id(0)
    span, width = emb.shape
    head = width // HEADS
    scale = 1.0 / math.sqrt(head)
    count = len_ref[half * half_seqs + step]
    block = span // 2

    def gate(raw, grad, weight):
        grown = jnp.exp(raw * (-scale))
        sigma = 1.0 / (1.0 + grown)
        act = raw * scale * sigma
        slope = sigma + act * (1.0 - sigma)
        return (
            (act * weight).astype(jnp.bfloat16),
            (grad * weight * slope).astype(jnp.bfloat16),
        )

    def run(live):
        base = pl.multiple_of(step * span, span)
        q_s[0:live, :] = dot(emb[0:live, :], wq[...]).astype(jnp.bfloat16)
        k_s[0:live, :] = dot(emb[0:live, :], wk[...]).astype(jnp.bfloat16)
        v_s[0:live, :] = dot(emb[0:live, :], wv[...]).astype(jnp.bfloat16)
        lane = lax.broadcasted_iota(jnp.int32, (1, block), 1)
        inverse = 1.0 / jnp.broadcast_to(count, (1, block)).astype(jnp.float32)
        sub = lax.broadcasted_iota(jnp.int32, (block, block), 0)
        lan = lax.broadcasted_iota(jnp.int32, (block, block), 1)
        causal = sub <= lan
        for h in range(HEADS):
            cols = slice(h * head, (h + 1) * head)
            att, sco = {}, {}
            for i in range(live // block):
                weight = jnp.where(lane + i * block < count, inverse, 0.0)
                iq = q_s[i * block:(i + 1) * block, cols]
                ig = gout[i * block:(i + 1) * block, cols]
                for j in range(i + 1):
                    jk = k_s[j * block:(j + 1) * block, cols]
                    jv = v_s[j * block:(j + 1) * block, cols]
                    raw = dot(jk, iq, NT)
                    grad = dot(jv, ig, NT)
                    if i == j:
                        use = jnp.where(causal, weight, 0.0)
                    else:
                        use = weight
                    att[j, i], sco[j, i] = gate(raw, grad, use)
            for j in range(live // block):
                vg = kg = None
                for i in range(j, live // block):
                    iq = q_s[i * block:(i + 1) * block, cols]
                    ig = gout[i * block:(i + 1) * block, cols]
                    a, b = dot(att[j, i], ig), dot(sco[j, i], iq)
                    vg = a if vg is None else vg + a
                    kg = b if kg is None else kg + b
                dv_s[j * block:(j + 1) * block, cols] = vg.astype(jnp.bfloat16)
                dk_s[j * block:(j + 1) * block, cols] = (kg * scale).astype(jnp.bfloat16)
            for i in range(live // block):
                qg = None
                for j in range(i + 1):
                    jk = k_s[j * block:(j + 1) * block, cols]
                    c = dot(sco[j, i], jk, TN)
                    qg = c if qg is None else qg + c
                dq_s[i * block:(i + 1) * block, cols] = (qg * scale).astype(jnp.bfloat16)
        token = dot(dq_s[0:live, :], wq[...], NT)
        token = token + dot(dk_s[0:live, :], wk[...], NT)
        token = token + dot(dv_s[0:live, :], wv[...], NT)
        tok_s[pl.ds(base, live), :] = token.astype(jnp.bfloat16)
        if live < span:
            tok_s[pl.ds(base + live, span - live), :] = jnp.zeros(
                (span - live, width), jnp.bfloat16
            )

    @pl.when(count <= block)
    def _():
        run(block)

    @pl.when(count > block)
    def _():
        run(span)

    @pl.when(step == pl.num_programs(0) - 1)
    def _():
        me = lax.axis_index("group")
        owned = half_tiles // groups
        halves = own_ref.shape[0] // half_tiles

        def place(part):
            for g in range(groups):
                idx_s[groups * owned + g] = 0
            for t in range(half_tiles):
                owner = own_ref[part * half_tiles + t]
                seen = idx_s[groups * owned + owner]
                idx_s[owner * owned + seen] = t
                idx_s[groups * owned + owner] = seen + 1

        if extra:
            total = len_ref[0]
            for s in range(1, len_ref.shape[0]):
                total = total + len_ref[s]
            for k in range(groups):
                ext_s[k] = jnp.zeros(ext_s.shape[1:], jnp.float32)
                ext_s[k, halves * owned:halves * owned + 1, :] = digits_row(total, width)
            for part in range(halves):
                place(part)
                for k in range(groups):
                    owner = me ^ k
                    for s in range(owned):
                        t = idx_s[owner * owned + s] + part * half_tiles
                        row = rows[pl.ds(t, 1), :]
                        at = part * owned + s
                        ext_s[k, at:at + 1, 0:tile] = (row // ROWS_DEV).astype(jnp.float32)
                        ext_s[k, at:at + 1, tile:2 * tile] = (row % ROWS_DEV).astype(jnp.float32)
            for k in range(groups):
                outs[k][owned * tile:owned * tile + EXTRA, :] = ext_s[k].astype(jnp.bfloat16)
        place(half)
        for k in range(groups):
            owner = me ^ k
            for s in range(owned):
                t = idx_s[owner * owned + s]
                outs[k][s * tile:(s + 1) * tile, :] = tok_s[
                    pl.ds(pl.multiple_of(t * tile, tile), tile), :
                ]


def attention(half, halves, groups, lengths, owners, embeds, out_grad, wq, wk, wv, rows, extra):
    tokens, width = embeds.shape
    seqs = lengths.shape[0]
    span = tokens // seqs
    tile = tokens // owners.shape[0]
    half_seqs, half_tiles = seqs // halves, owners.shape[0] // halves
    owned = half_tiles // groups
    out_rows = owned * tile + (EXTRA if extra else 0)
    whole = lambda s: (0, 0)
    smem = pl.BlockSpec(memory_space=pltpu.SMEM)
    flops = half_seqs * (2 * span * width * width * 6 + 10 * span * span * width)
    return pl.pallas_call(
        functools.partial(attention_kernel, half, half_seqs, half_tiles, groups, tile, extra),
        grid=(half_seqs,),
        in_specs=[
            smem, smem,
            pl.BlockSpec((span, width), lambda s: (half * half_seqs + s, 0)),
            pl.BlockSpec((span, width), lambda s: (half * half_seqs + s, 0)),
            pl.BlockSpec((width, width), whole),
            pl.BlockSpec((width, width), whole),
            pl.BlockSpec((width, width), whole),
            pl.BlockSpec((owners.shape[0], tile), whole),
        ],
        out_specs=[pl.BlockSpec((out_rows, width), whole)] * groups,
        out_shape=[jax.ShapeDtypeStruct((out_rows, width), jnp.bfloat16)] * groups,
        scratch_shapes=[pltpu.VMEM((span, width), jnp.bfloat16)] * 6 + [
            pltpu.VMEM((half_seqs * span, width), jnp.bfloat16),
            pltpu.VMEM((groups, EXTRA, width), jnp.float32),
            pltpu.SMEM((groups * owned + groups,), jnp.int32),
        ],
        cost_estimate=pl.CostEstimate(
            flops=flops, bytes_accessed=4 * half_seqs * span * width * 2, transcendentals=0
        ),
        name=f"attention_{half}",
    )(lengths, owners, embeds, out_grad, wq, wk, wv, rows)


def keys_of(ext, slots, tile):
    high = jnp.concatenate([e[s:s + 1, 0:tile] for e, s in slots], axis=1)
    low = jnp.concatenate([e[s:s + 1, tile:2 * tile] for e, s in slots], axis=1)
    return high, low


def sums_of(block, boxes, exts, first, owned, tile):
    total = None
    row = lax.broadcasted_iota(jnp.int32, (ROWS_DEV, owned * tile), 0).astype(jnp.float32)
    for box, ext in zip(boxes, exts):
        high = jnp.concatenate(
            [ext[first + s:first + s + 1, 0:tile] for s in range(owned)], axis=1
        ).astype(jnp.float32)
        low = jnp.concatenate(
            [ext[first + s:first + s + 1, tile:2 * tile] for s in range(owned)], axis=1
        ).astype(jnp.float32)
        key = jnp.where(high == block.astype(jnp.float32), low, -1.0)
        hot = jnp.where(row == key, 1.0, 0.0).astype(jnp.bfloat16)
        part = dot(hot, box[0:owned * tile, :])
        total = part if total is None else total + part
    return total


def first_kernel(pairs, owned, tile, *refs):
    boxes, acc = refs[:-1], refs[-1]
    core = lax.axis_index("batch") % 2
    base = owned * tile
    exts = [b[base:base + EXTRA, :] for b in boxes]
    for side in range(2):
        for p in range(pairs):
            block = 2 * p + (1 - core if side == 0 else core)
            acc[side, p] = sums_of(block, boxes, exts, 0, owned, tile)


def live_of(exts, at):
    total = None
    for e in exts:
        row = total_of_digits(e[at:at + 1, :].astype(jnp.float32))
        total = row if total is None else total + row
    return total


def digits_of_float(total, width):
    return digits_row(jnp.broadcast_to(total, (1, width)).astype(jnp.int32), width)


def second_kernel(side, pairs, owned, tile, groups, *refs):
    boxes, firsts, acc, out = refs[:groups], refs[groups:2 * groups], refs[-2], refs[-1]
    core = lax.axis_index("batch") % 2
    base = owned * tile
    exts = [b[base:base + EXTRA, :] for b in firsts]
    width = out.shape[-1]
    for p in range(pairs):
        block = 2 * p + (1 - core if side == 0 else core)
        total = acc[0, p] + sums_of(block, boxes, exts, owned, owned, tile)
        out[p * ROWS_DEV:(p + 1) * ROWS_DEV, :] = total.astype(out.dtype)
    if side == 0:
        live = live_of(exts, 2 * owned)
        row = digits_of_float(live, width)
        out[pairs * ROWS_DEV:pairs * ROWS_DEV + EXTRA, :] = jnp.broadcast_to(
            row, (EXTRA, width)
        ).astype(out.dtype)


def pair_kernel(pairs, owned, tile, groups, *refs):
    firsts, own, got = refs[:groups], refs[groups], refs[groups + 1]
    outs = refs[groups + 2:]
    pair = lax.axis_index("batch") // 2
    base = owned * tile
    width = own.shape[-1]
    live = live_of([b[base:base + EXTRA, :] for b in firsts], 2 * owned)
    other = total_of_digits(got[pairs * ROWS_DEV:pairs * ROWS_DEV + 1, :].astype(jnp.float32))
    both = digits_of_float(live + other, width)
    for k in range(pairs):
        at = pl.multiple_of((pair ^ k) * ROWS_DEV, ROWS_DEV)
        total = own[pl.ds(at, ROWS_DEV), :] + got[pl.ds(at, ROWS_DEV), :].astype(jnp.float32)
        outs[k][0:ROWS_DEV, :] = total.astype(outs[k].dtype)
        outs[k][ROWS_DEV:ROWS_DEV + EXTRA, :] = jnp.broadcast_to(both, (EXTRA, width)).astype(
            outs[k].dtype
        )


def last_kernel(tokens_all, *refs):
    ins, out = refs[:-1], refs[-1]
    total = live = None
    for r in ins:
        part = r[0:ROWS_DEV, :].astype(jnp.float32)
        some = total_of_digits(r[ROWS_DEV:ROWS_DEV + 1, :].astype(jnp.float32))
        total = part if total is None else total + part
        live = some if live is None else live + some
    out[...] = total * (tokens_all / live)


def vmem(n):
    return [pl.BlockSpec(memory_space=pltpu.VMEM)] * n


def on_device(groups, batches, embeds, out_grad, w_query, w_key, w_value, lengths, item_rows,
              tile_owner):
    tokens, width = embeds.shape
    halves = 2
    tile = tokens // tile_owner.shape[0]
    owned = tile_owner.shape[0] // halves // groups
    pairs = batches // 2
    rows = item_rows.reshape(-1, tile)
    f32, bf16 = jnp.float32, jnp.bfloat16

    def swap(box, k):
        return lax.ppermute(box, "group", [(i, i ^ k) for i in range(groups)])

    boxes = []
    for half in range(halves):
        mine = attention(
            half, halves, groups, lengths, tile_owner, embeds, out_grad,
            w_query, w_key, w_value, rows, half == 0,
        )
        boxes.append([mine[0]] + [swap(mine[k], k) for k in range(1, groups)])

    def call(kernel, shapes, name, flops, *args):
        return pl.pallas_call(
            kernel,
            in_specs=vmem(len(args)),
            out_specs=vmem(len(shapes)) if isinstance(shapes, list) else vmem(1)[0],
            out_shape=shapes,
            cost_estimate=pl.CostEstimate(flops=flops, bytes_accessed=1 << 20, transcendentals=0),
            name=name,
        )(*args)

    shape = jax.ShapeDtypeStruct
    work = 2 * pairs * ROWS_DEV * width * owned * tile * groups
    acc = call(
        functools.partial(first_kernel, pairs, owned, tile),
        shape((2, pairs, ROWS_DEV, width), f32), "sums_first", 2 * work, *boxes[0],
    )

    def second(side, out):
        return pl.pallas_call(
            functools.partial(second_kernel, side, pairs, owned, tile, groups),
            grid=(1,),
            in_specs=vmem(2 * groups) + [
                pl.BlockSpec((1, pairs, ROWS_DEV, width), lambda s: (side, 0, 0, 0))
            ],
            out_specs=vmem(1)[0],
            out_shape=out,
            cost_estimate=pl.CostEstimate(
                flops=work, bytes_accessed=1 << 20, transcendentals=0
            ),
            name=f"sums_second_{side}",
        )(*boxes[1], *boxes[0], acc)

    send = second(0, shape((pairs * ROWS_DEV + EXTRA, width), bf16))
    got = lax.ppermute(send, "batch", [(i, i ^ 1) for i in range(batches)])
    own = second(1, shape((pairs * ROWS_DEV, width), f32))
    parts = call(
        functools.partial(pair_kernel, pairs, owned, tile, groups),
        [shape((ROWS_DEV + EXTRA, width), f32 if k == 0 else bf16) for k in range(pairs)],
        "pair_sums", 1 << 22, *boxes[0], own, got,
    )
    ends = [parts[0]] + [
        lax.ppermute(parts[k], "batch", [(i, i ^ (2 * k)) for i in range(batches)])
        for k in range(1, pairs)
    ]
    tokens_all = float(tokens * groups * batches)
    return call(
        functools.partial(last_kernel, tokens_all),
        shape((ROWS_DEV, width), f32), "final", 1 << 20, *ends,
    )


def solution(mesh):
    groups, batches = mesh.shape["group"], mesh.shape["batch"]
    both = P(("group", "batch"))
    wide = P(("group", "batch"), None)
    return jax.shard_map(
        functools.partial(on_device, groups, batches),
        mesh=mesh,
        in_specs=(wide, wide, P(), P(), P(), both, both, both),
        out_specs=wide,
        check_vma=False,
    )
```

```python
import functools
import math

import jax
import jax.numpy as jnp
from jax import lax
from jax.experimental import pallas as pl
from jax.experimental.pallas import tpu as pltpu
from jax.sharding import PartitionSpec as P


HEADS = 2
ROWS_DEV = 256
EXTRA = 8
BASE = 128
LIMIT = 24 << 20
NT = (((1,), (1,)), ((), ()))
TN = (((0,), (0,)), ((), ()))


def dot(a, b, dims=(((1,), (0,)), ((), ()))):
    return lax.dot_general(a, b, dims, preferred_element_type=jnp.float32)


def digits_row(total, width):
    lane = lax.broadcasted_iota(jnp.int32, (1, width), 1)
    low, mid, high = total % BASE, (total // BASE) % BASE, total // (BASE * BASE)
    row = jnp.where(lane == 0, low, jnp.where(lane == 1, mid, jnp.where(lane == 2, high, 0)))
    return row.astype(jnp.float32)


def total_of_digits(row):
    return row[:, 0:1] + row[:, 1:2] * float(BASE) + row[:, 2:3] * float(BASE * BASE)


def attention_kernel(
    half, halves, groups, tile, extra,
    len_h, own_h, emb_h, gout_h, wq_h, wk_h, wv_h, rows_h, *refs,
):
    outs = refs[:groups]
    (emb, gout, wq, wk, wv, rows, len_ref, own_ref,
     q_s, k_s, v_s, dq_s, dk_s, dv_s, tok_s, ext_s, idx_s, sems) = refs[groups:]
    width = emb.shape[1]
    half_seqs = len_ref.shape[0] // halves
    half_tiles = own_ref.shape[0] // halves
    span = emb.shape[0] // half_seqs
    head = width // HEADS
    scale = 1.0 / math.sqrt(head)
    block = span // 2
    start = half * half_seqs * span

    def piece(s):
        return pl.ds(s * span, span)

    plan = [(len_h, len_ref)]
    plan += [(emb_h.at[pl.ds(start, span)], emb.at[piece(0)]), (wq_h, wq), (wk_h, wk), (wv_h, wv)]
    plan += [(gout_h.at[pl.ds(start, span)], gout.at[piece(0)])]
    for s in range(1, half_seqs):
        plan += [
            (emb_h.at[pl.ds(start + s * span, span)], emb.at[piece(s)]),
            (gout_h.at[pl.ds(start + s * span, span)], gout.at[piece(s)]),
        ]
    plan += [(own_h, own_ref), (rows_h, rows)]
    copies = [pltpu.make_async_copy(a, b, sems.at[i]) for i, (a, b) in enumerate(plan)]
    for c in copies:
        c.start()

    def gate(raw, grad, weight):
        grown = jnp.exp(raw * (-scale))
        sigma = 1.0 / (1.0 + grown)
        act = raw * scale * sigma
        slope = sigma + act * (1.0 - sigma)
        return (
            (act * weight).astype(jnp.bfloat16),
            (grad * weight * slope).astype(jnp.bfloat16),
        )

    def run(base, count, live):
        def rows_of(ref, at, size):
            return ref[base + at:base + at + size, :]

        q_s[0:live, :] = dot(rows_of(emb, 0, live), wq[...]).astype(jnp.bfloat16)
        k_s[0:live, :] = dot(rows_of(emb, 0, live), wk[...]).astype(jnp.bfloat16)
        v_s[0:live, :] = dot(rows_of(emb, 0, live), wv[...]).astype(jnp.bfloat16)
        lane = lax.broadcasted_iota(jnp.int32, (1, block), 1)
        inverse = 1.0 / jnp.broadcast_to(count, (1, block)).astype(jnp.float32)
        sub = lax.broadcasted_iota(jnp.int32, (block, block), 0)
        lan = lax.broadcasted_iota(jnp.int32, (block, block), 1)
        causal = sub <= lan
        for h in range(HEADS):
            cols = slice(h * head, (h + 1) * head)
            att, sco = {}, {}
            for i in range(live // block):
                weight = jnp.where(lane + i * block < count, inverse, 0.0)
                iq = q_s[i * block:(i + 1) * block, cols]
                ig = gout[base + i * block:base + (i + 1) * block, cols]
                for j in range(i + 1):
                    jk = k_s[j * block:(j + 1) * block, cols]
                    jv = v_s[j * block:(j + 1) * block, cols]
                    raw = dot(jk, iq, NT)
                    grad = dot(jv, ig, NT)
                    if i == j:
                        use = jnp.where(causal, weight, 0.0)
                    else:
                        use = weight
                    att[j, i], sco[j, i] = gate(raw, grad, use)
            for j in range(live // block):
                vg = kg = None
                for i in range(j, live // block):
                    iq = q_s[i * block:(i + 1) * block, cols]
                    ig = gout[base + i * block:base + (i + 1) * block, cols]
                    a, b = dot(att[j, i], ig), dot(sco[j, i], iq)
                    vg = a if vg is None else vg + a
                    kg = b if kg is None else kg + b
                dv_s[j * block:(j + 1) * block, cols] = vg.astype(jnp.bfloat16)
                dk_s[j * block:(j + 1) * block, cols] = (kg * scale).astype(jnp.bfloat16)
            for i in range(live // block):
                qg = None
                for j in range(i + 1):
                    jk = k_s[j * block:(j + 1) * block, cols]
                    c = dot(sco[j, i], jk, TN)
                    qg = c if qg is None else qg + c
                dq_s[i * block:(i + 1) * block, cols] = (qg * scale).astype(jnp.bfloat16)
        token = dot(dq_s[0:live, :], wq[...], NT)
        token = token + dot(dk_s[0:live, :], wk[...], NT)
        token = token + dot(dv_s[0:live, :], wv[...], NT)
        tok_s[base:base + live, :] = token.astype(jnp.bfloat16)
        if live < span:
            tok_s[base + live:base + span, :] = jnp.zeros((span - live, width), jnp.bfloat16)

    for c in copies[:6]:
        c.wait()
    for s in range(half_seqs):
        if s:
            for c in copies[4 + 2 * s:6 + 2 * s]:
                c.wait()
        count = len_ref[half * half_seqs + s]
        pl.when(count <= block)(functools.partial(run, s * span, count, block))
        pl.when(count > block)(functools.partial(run, s * span, count, span))
    for c in copies[-2:]:
        c.wait()

    me = lax.axis_index("group")
    owned = half_tiles // groups

    def place(part):
        for g in range(groups):
            idx_s[groups * owned + g] = 0
        for t in range(half_tiles):
            owner = own_ref[part * half_tiles + t]
            seen = idx_s[groups * owned + owner]
            idx_s[owner * owned + seen] = t
            idx_s[groups * owned + owner] = seen + 1

    if extra:
        total = len_ref[0]
        for s in range(1, len_ref.shape[0]):
            total = total + len_ref[s]
        for k in range(groups):
            ext_s[k] = jnp.zeros(ext_s.shape[1:], jnp.float32)
            ext_s[k, halves * owned:halves * owned + 1, :] = digits_row(total, width)
        for part in range(halves):
            place(part)
            for k in range(groups):
                owner = me ^ k
                for s in range(owned):
                    t = idx_s[owner * owned + s] + part * half_tiles
                    row = rows[pl.ds(t, 1), :]
                    at = part * owned + s
                    ext_s[k, at:at + 1, 0:tile] = (row // ROWS_DEV).astype(jnp.float32)
                    ext_s[k, at:at + 1, tile:2 * tile] = (row % ROWS_DEV).astype(jnp.float32)
        for k in range(groups):
            outs[k][owned * tile:owned * tile + EXTRA, :] = ext_s[k].astype(jnp.bfloat16)
    place(half)
    for k in range(groups):
        owner = me ^ k
        for s in range(owned):
            t = idx_s[owner * owned + s]
            outs[k][s * tile:(s + 1) * tile, :] = tok_s[
                pl.ds(pl.multiple_of(t * tile, tile), tile), :
            ]


def attention(half, halves, groups, lengths, owners, embeds, out_grad, wq, wk, wv, rows, extra):
    tokens, width = embeds.shape
    seqs = lengths.shape[0]
    span = tokens // seqs
    tile = tokens // owners.shape[0]
    half_seqs, half_tiles = seqs // halves, owners.shape[0] // halves
    owned = half_tiles // groups
    out_rows = owned * tile + (EXTRA if extra else 0)
    flops = half_seqs * (2 * span * width * width * 6 + 10 * span * span * width)
    bf16 = jnp.bfloat16
    return pl.pallas_call(
        functools.partial(attention_kernel, half, halves, groups, tile, extra),
        in_specs=[pl.BlockSpec(memory_space=pltpu.HBM)] * 8,
        out_specs=vmem(groups),
        out_shape=[jax.ShapeDtypeStruct((out_rows, width), bf16)] * groups,
        scratch_shapes=[pltpu.VMEM((half_seqs * span, width), bf16)] * 2
        + [pltpu.VMEM((width, width), bf16)] * 3
        + [
            pltpu.VMEM(rows.shape, jnp.int32),
            pltpu.SMEM(lengths.shape, jnp.int32),
            pltpu.SMEM(owners.shape, jnp.int32),
        ]
        + [pltpu.VMEM((span, width), bf16)] * 6
        + [
            pltpu.VMEM((half_seqs * span, width), bf16),
            pltpu.VMEM((groups, EXTRA, width), jnp.float32),
            pltpu.SMEM((groups * owned + groups,), jnp.int32),
            pltpu.SemaphoreType.DMA((6 + 2 * half_seqs,)),
        ],
        compiler_params=pltpu.CompilerParams(vmem_limit_bytes=LIMIT),
        cost_estimate=pl.CostEstimate(
            flops=flops, bytes_accessed=4 * half_seqs * span * width * 2, transcendentals=0
        ),
    )(*[
        pltpu.with_memory_space_constraint(a, pltpu.HBM)
        for a in (lengths, owners, embeds, out_grad, wq, wk, wv, rows)
    ])


def sums_of(block, boxes, exts, first, owned, tile):
    total = None
    row = lax.broadcasted_iota(jnp.int32, (ROWS_DEV, owned * tile), 0).astype(jnp.float32)
    for box, ext in zip(boxes, exts):
        slots = [ext[first + s:first + s + 1, :].astype(jnp.float32) for s in range(owned)]
        high = jnp.concatenate([r[:, 0:tile] for r in slots], axis=1)
        low = jnp.concatenate([r[:, tile:2 * tile] for r in slots], axis=1)
        key = jnp.where(high == block.astype(jnp.float32), low, -1.0)
        hot = jnp.where(row == key, 1.0, 0.0).astype(jnp.bfloat16)
        part = dot(hot, box[0:owned * tile, :])
        total = part if total is None else total + part
    return total


def live_of(exts, at):
    total = None
    for e in exts:
        row = total_of_digits(e[at:at + 1, :].astype(jnp.float32))
        total = row if total is None else total + row
    return total


def live_rows(total, like):
    width = like.shape[-1]
    row = digits_row(jnp.broadcast_to(total, (1, width)).astype(jnp.int32), width)
    return jnp.broadcast_to(row, (EXTRA, width)).astype(like.dtype)


def exts_of(boxes, base):
    return [b[base:base + EXTRA, :] for b in boxes]


def first_kernel(pairs, owned, tile, *refs):
    boxes, acc = refs[:-1], refs[-1]
    core = lax.axis_index("batch") % 2
    exts = exts_of(boxes, owned * tile)
    for side in range(2):
        for p in range(pairs):
            block = 2 * p + (1 - core if side == 0 else core)
            acc[side, p] = sums_of(block, boxes, exts, 0, owned, tile)


def side_kernel(side, pairs, owned, tile, heads, bodies, *refs):
    acc = refs[heads + bodies] if len(refs) > heads + bodies + 1 else None
    head, body, out = refs[:heads], refs[heads:heads + bodies], refs[-1]
    core = lax.axis_index("batch") % 2
    exts = exts_of(head, owned * tile)
    for p in range(pairs):
        block = 2 * p + (1 - core if side == 0 else core)
        total = sums_of(block, body, exts, owned, owned, tile)
        if acc is None:
            total = total + sums_of(block, head, exts, 0, owned, tile)
        else:
            total = total + acc[0, p]
        out[p * ROWS_DEV:(p + 1) * ROWS_DEV, :] = total.astype(out.dtype)
    if side == 0:
        out[pairs * ROWS_DEV:pairs * ROWS_DEV + EXTRA, :] = live_rows(
            live_of(exts, 2 * owned), out
        )


def pair_kernel(pairs, owned, tile, heads, *refs):
    head, own, got = refs[:heads], refs[heads], refs[heads + 1]
    outs = refs[heads + 2:]
    pair = lax.axis_index("batch") // 2
    live = live_of(exts_of(head, owned * tile), 2 * owned)
    live = live + live_of([got[pairs * ROWS_DEV:pairs * ROWS_DEV + 1, :]], 0)
    for k in range(pairs):
        at = pl.multiple_of((pair ^ k) * ROWS_DEV, ROWS_DEV)
        total = own[pl.ds(at, ROWS_DEV), :] + got[pl.ds(at, ROWS_DEV), :].astype(jnp.float32)
        outs[k][0:ROWS_DEV, :] = total.astype(outs[k].dtype)
        outs[k][ROWS_DEV:ROWS_DEV + EXTRA, :] = live_rows(live, outs[k])


def gathered(ins):
    total = live = None
    for r in ins:
        part = r[0:ROWS_DEV, :].astype(jnp.float32)
        some = total_of_digits(r[ROWS_DEV:ROWS_DEV + 1, :].astype(jnp.float32))
        total = part if total is None else total + part
        live = some if live is None else live + some
    return total, live


def far_kernel(*refs):
    total, live = gathered(refs[:-1])
    out = refs[-1]
    out[0:ROWS_DEV, :] = total.astype(out.dtype)
    out[ROWS_DEV:ROWS_DEV + EXTRA, :] = live_rows(live, out)


def last_kernel(tokens_all, *refs):
    total, live = gathered(refs[:-1])
    refs[-1][...] = total * (tokens_all / live)


def vmem(n):
    return [pl.BlockSpec(memory_space=pltpu.VMEM)] * n


def call(kernel, shapes, flops, *args):
    return pl.pallas_call(
        kernel,
        in_specs=vmem(len(args)),
        out_specs=vmem(len(shapes)) if isinstance(shapes, list) else vmem(1)[0],
        out_shape=shapes,
        compiler_params=pltpu.CompilerParams(vmem_limit_bytes=LIMIT),
        cost_estimate=pl.CostEstimate(flops=flops, bytes_accessed=1 << 20, transcendentals=0),
    )(*args)


def on_device(groups, batches, embeds, out_grad, w_query, w_key, w_value, lengths, item_rows,
              tile_owner):
    tokens, width = embeds.shape
    halves = 2
    tile = tokens // tile_owner.shape[0]
    owned = tile_owner.shape[0] // halves // groups
    pairs = batches // 2
    rows = item_rows.reshape(-1, tile)
    f32, bf16 = jnp.float32, jnp.bfloat16
    shape = jax.ShapeDtypeStruct
    far = groups - 1
    work = 2 * pairs * ROWS_DEV * width * owned * tile

    def swap(box, k):
        return lax.ppermute(box, "group", [(i, i ^ k) for i in range(groups)])

    def across(box, k):
        return lax.ppermute(box, "batch", [(i, i ^ k) for i in range(batches)])

    near, away = [], []
    for half in range(halves):
        mine = list(attention(
            half, halves, groups, lengths, tile_owner, embeds, out_grad,
            w_query, w_key, w_value, rows, half == 0,
        ))
        near.append([mine[0]] + [swap(mine[k], k) for k in range(far - 1, 0, -1)])
        away.append([mine[far]])

    def side(which, flops, heads, bodies, acc=None):
        out = shape((pairs * ROWS_DEV + EXTRA, width), bf16) if which == 0 else shape(
            (pairs * ROWS_DEV, width), f32)
        specs = vmem(len(heads) + len(bodies))
        args = [*heads, *bodies]
        if acc is not None:
            specs = specs + [
                pl.BlockSpec((1, pairs, ROWS_DEV, width), lambda s: (which, 0, 0, 0))
            ]
            args = args + [acc]
        return pl.pallas_call(
            functools.partial(
                side_kernel, which, pairs, owned, tile, len(heads), len(bodies)
            ),
            grid=(1,),
            in_specs=specs,
            out_specs=vmem(1)[0],
            out_shape=out,
            compiler_params=pltpu.CompilerParams(vmem_limit_bytes=LIMIT),
            cost_estimate=pl.CostEstimate(
                flops=flops, bytes_accessed=1 << 20, transcendentals=0
            ),
        )(*args)

    def plane(heads, bodies, acc=None):
        flops = work * (len(bodies) + (len(heads) if acc is None else 0))
        send = side(0, flops, heads, bodies, acc)
        got = across(send, 1)
        own = side(1, flops, heads, bodies, acc)
        parts = call(
            functools.partial(pair_kernel, pairs, owned, tile, len(heads)),
            [shape((ROWS_DEV + EXTRA, width), f32 if k == 0 else bf16) for k in range(pairs)],
            1 << 22, *heads, own, got,
        )
        return [parts[0]] + [across(parts[k], 2 * k) for k in range(1, pairs)]

    far_parts = plane(away[0], away[1])
    acc = call(
        functools.partial(first_kernel, pairs, owned, tile),
        shape((2, pairs, ROWS_DEV, width), f32), 2 * far * work, *near[0],
    )
    near_parts = plane(near[0], near[1], acc)
    far_sum = call(far_kernel, shape((ROWS_DEV + EXTRA, width), bf16), 1 << 20, *far_parts)
    return call(
        functools.partial(last_kernel, float(tokens * groups * batches)),
        shape((ROWS_DEV, width), f32), 1 << 20, *near_parts, swap(far_sum, far),
    )


def solution(mesh):
    groups, batches = mesh.shape["group"], mesh.shape["batch"]
    both = P(("group", "batch"))
    wide = P(("group", "batch"), None)

    def body(*args):
        return on_device(groups, batches, *args)

    return jax.shard_map(
        body,
        mesh=mesh,
        in_specs=(wide, wide, P(), P(), P(), both, both, both),
        out_specs=wide,
        check_vma=False,
    )
```

```python
import functools
import math

import jax
import jax.numpy as jnp
from jax import lax
from jax.experimental import pallas as pl
from jax.experimental.pallas import tpu as pltpu
from jax.sharding import PartitionSpec as P


HEADS = 2
ROWS_DEV = 256
EXTRA = 8
BASE = 128
LIMIT = 24 << 20
NT = (((1,), (1,)), ((), ()))
TN = (((0,), (0,)), ((), ()))


def dot(a, b, dims=(((1,), (0,)), ((), ()))):
    return lax.dot_general(a, b, dims, preferred_element_type=jnp.float32)


def digits_row(total, width):
    lane = lax.broadcasted_iota(jnp.int32, (1, width), 1)
    low, mid, high = total % BASE, (total // BASE) % BASE, total // (BASE * BASE)
    row = jnp.where(lane == 0, low, jnp.where(lane == 1, mid, jnp.where(lane == 2, high, 0)))
    return row.astype(jnp.float32)


def total_of_digits(row):
    return row[:, 0:1] + row[:, 1:2] * float(BASE) + row[:, 2:3] * float(BASE * BASE)


def attention_kernel(half, halves, groups, tile, len_h, own_h, *refs):
    first = half == 0
    if first:
        (emb_h, gout_h, wq_h, wk_h, wv_h, rows_h), refs = refs[:6], refs[6:]
        outs, refs = refs[:groups], refs[groups:]
        (wq, wk, wv, emb_next, gout_next, counts), refs = refs[:6], refs[6:]
        (emb, gout, rows), refs = refs[:3], refs[3:]
    else:
        (emb, gout, wq, wk, wv, counts, kept), refs = refs[:7], refs[7:]
        outs, refs = refs[:groups], refs[groups:]
    len_ref, own_ref, q_s, k_s, v_s, dq_s, dk_s, dv_s, tok_s, ext_s, idx_s, sems = refs
    width = emb.shape[1]
    half_seqs = len_ref.shape[0] // halves
    half_tiles = own_ref.shape[0] // halves
    owned = half_tiles // groups
    size = emb.shape[0]
    span = size // half_seqs
    head = width // HEADS
    scale = 1.0 / math.sqrt(head)
    block = span // 2
    sub = block // 2

    def load(source, target, sem):
        return pltpu.make_async_copy(source, target, sem)

    def load_rows(source, target, base, at, count, sem):
        return load(source.at[pl.ds(base + at, count)], target.at[pl.ds(at, count)], sem)

    wait_len, wait_own = load(len_h, len_ref, sems.at[0]), load(own_h, own_ref, sems.at[1])
    if first:
        wait_len.start()
        head_loads = [load(wq_h, wq, sems.at[2]), load(wk_h, wk, sems.at[3])]
        head_loads += [load(wv_h, wv, sems.at[4])]
        wait_rows = load(rows_h, rows, sems.at[5])

        def loads(s):
            low = load_rows(emb_h, emb, 0, s * span, block, sems.at[8 + 3 * s])
            high = load_rows(emb_h, emb, 0, s * span + block, block, sems.at[9 + 3 * s])
            other = load_rows(gout_h, gout, 0, s * span, span, sems.at[10 + 3 * s])
            return low, high, other

        for s in range(half_seqs):
            low, high, other = loads(s)
            low.start()
            if s == 0:
                for c in head_loads:
                    c.start()
            high.start()
            other.start()
        wait_rows.start()
        later = [
            load_rows(emb_h, emb_next, size, 0, size, sems.at[6]),
            load_rows(gout_h, gout_next, size, 0, size, sems.at[7]),
        ]
    wait_own.start()

    def gate(raw, grad, weight):
        grown = jnp.exp(raw * (-scale))
        sigma = 1.0 / (1.0 + grown)
        act = raw * scale * sigma
        slope = sigma + act * (1.0 - sigma)
        return (
            (act * weight).astype(jnp.bfloat16),
            (grad * weight * slope).astype(jnp.bfloat16),
        )

    def project(base, at):
        rows_in = emb[pl.ds(base + at, block), :]
        q_s[at:at + block, :] = dot(rows_in, wq[...]).astype(jnp.bfloat16)
        k_s[at:at + block, :] = dot(rows_in, wk[...]).astype(jnp.bfloat16)
        v_s[at:at + block, :] = dot(rows_in, wv[...]).astype(jnp.bfloat16)

    def run(base, count, live):
        if live > block:
            project(base, block)
        lane = lax.broadcasted_iota(jnp.int32, (1, block), 1)
        inverse = 1.0 / jnp.broadcast_to(count, (1, block)).astype(jnp.float32)
        causal = lax.broadcasted_iota(jnp.int32, (sub, sub), 0) <= lax.broadcasted_iota(
            jnp.int32, (sub, sub), 1
        )
        zeros = jnp.zeros((sub, sub), jnp.bfloat16)
        for h in range(HEADS):
            cols = slice(h * head, (h + 1) * head)
            att, sco = {}, {}
            for i in range(live // block):
                weight = jnp.where(lane + i * block < count, inverse, 0.0)
                iq = q_s[i * block:(i + 1) * block, cols]
                ig = gout[pl.ds(base + i * block, block), cols]
                for j in range(i + 1):
                    jk = k_s[j * block:(j + 1) * block, cols]
                    jv = v_s[j * block:(j + 1) * block, cols]
                    raw = dot(jk, iq, NT)
                    grad = dot(jv, ig, NT)
                    if i != j:
                        att[j, i], sco[j, i] = gate(raw, grad, weight)
                        continue
                    low, high = weight[:, :sub], weight[:, sub:]
                    a0, s0 = gate(
                        raw[:sub, :sub], grad[:sub, :sub], jnp.where(causal, low, 0.0)
                    )
                    a1, s1 = gate(raw[:sub, sub:], grad[:sub, sub:], high)
                    a2, s2 = gate(
                        raw[sub:, sub:], grad[sub:, sub:], jnp.where(causal, high, 0.0)
                    )

                    def whole(x, y, z):
                        return jnp.concatenate(
                            [
                                jnp.concatenate([x, y], axis=1),
                                jnp.concatenate([zeros, z], axis=1),
                            ],
                            axis=0,
                        )

                    att[j, i], sco[j, i] = whole(a0, a1, a2), whole(s0, s1, s2)
            for j in range(live // block):
                vg = kg = None
                for i in range(j, live // block):
                    iq = q_s[i * block:(i + 1) * block, cols]
                    ig = gout[pl.ds(base + i * block, block), cols]
                    a, b = dot(att[j, i], ig), dot(sco[j, i], iq)
                    vg = a if vg is None else vg + a
                    kg = b if kg is None else kg + b
                dv_s[j * block:(j + 1) * block, cols] = vg.astype(jnp.bfloat16)
                dk_s[j * block:(j + 1) * block, cols] = (kg * scale).astype(jnp.bfloat16)
            for i in range(live // block):
                qg = None
                for j in range(i + 1):
                    jk = k_s[j * block:(j + 1) * block, cols]
                    c = dot(sco[j, i], jk, TN)
                    qg = c if qg is None else qg + c
                dq_s[i * block:(i + 1) * block, cols] = (qg * scale).astype(jnp.bfloat16)
        token = dot(dq_s[0:live, :], wq[...], NT)
        token = token + dot(dk_s[0:live, :], wk[...], NT)
        token = token + dot(dv_s[0:live, :], wv[...], NT)
        tok_s[pl.ds(base, live), :] = token.astype(jnp.bfloat16)
        if live < span:
            tok_s[pl.ds(base + live, span - live), :] = jnp.zeros((span - live, width), jnp.bfloat16)

    if first:
        for c in head_loads:
            c.wait()
        wait_len.wait()
        for s in range(len_ref.shape[0]):
            counts[s:s + 1, :] = jnp.broadcast_to(len_ref[s], (1, counts.shape[1]))

    def one(s, carry):
        base = pl.multiple_of(s * span, span)
        if first:
            low, high, other = loads(s)
            low.wait()
        project(base, 0)
        if first:
            high.wait()
            other.wait()

            @pl.when(s == half_seqs - 1)
            def _():
                for c in later:
                    c.start()

        if first:
            count = len_ref[half * half_seqs + s]
        else:
            count = jnp.max(counts[pl.ds(half * half_seqs + s, 1), :])
        pl.when(count <= block)(functools.partial(run, base, count, block))
        pl.when(count > block)(functools.partial(run, base, count, span))
        return carry

    lax.fori_loop(0, half_seqs, one, 0)
    wait_own.wait()

    me = lax.axis_index("group")

    def place(part):
        for g in range(groups):
            idx_s[groups * owned + g] = 0
        for t in range(half_tiles):
            owner = own_ref[part * half_tiles + t]
            seen = idx_s[groups * owned + owner]
            idx_s[owner * owned + seen] = t
            idx_s[groups * owned + owner] = seen + 1

    if first:
        wait_rows.wait()
        total = len_ref[0]
        for s in range(1, len_ref.shape[0]):
            total = total + len_ref[s]
        for k in range(groups):
            ext_s[k] = jnp.zeros(ext_s.shape[1:], jnp.float32)
            ext_s[k, halves * owned:halves * owned + 1, :] = digits_row(total, width)
        for part in range(halves - 1, -1, -1):
            place(part)
            for k in range(groups):
                owner = me ^ k
                for s in range(owned):
                    t = idx_s[owner * owned + s] + part * half_tiles
                    row = rows[pl.ds(t, 1), :]
                    at = part * owned + s
                    ext_s[k, at:at + 1, 0:tile] = (row // ROWS_DEV).astype(jnp.float32)
                    ext_s[k, at:at + 1, tile:2 * tile] = (row % ROWS_DEV).astype(jnp.float32)
        for k in range(groups):
            outs[k][owned * tile:owned * tile + EXTRA, :] = ext_s[k].astype(jnp.bfloat16)
    else:
        place(half)
    for k in range(groups):
        owner = me ^ k
        shift = 0
        if not first and k == groups - 1:
            shift = owned * tile
            outs[k][0:shift, :] = kept[0:shift, :]
            outs[k][2 * shift:2 * shift + EXTRA, :] = kept[shift:shift + EXTRA, :]
        for s in range(owned):
            t = idx_s[owner * owned + s]
            outs[k][shift + s * tile:shift + (s + 1) * tile, :] = tok_s[
                pl.ds(pl.multiple_of(t * tile, tile), tile), :
            ]
    if first:
        for c in later:
            c.wait()


def attention(half, halves, groups, lengths, owners, *given):
    width = given[0].shape[1]
    first = half == 0
    size = given[0].shape[0] // (halves if first else 1)
    seqs, tiles = lengths.shape[0], owners.shape[0]
    span = size * halves // seqs
    tile = size * halves // tiles
    half_seqs, half_tiles = seqs // halves, tiles // halves
    owned = half_tiles // groups
    bf16 = jnp.bfloat16
    box = owned * tile
    flops = half_seqs * (2 * span * width * width * 6 + 10 * span * span * width)
    hbm = pl.BlockSpec(memory_space=pltpu.HBM)
    scratch = []
    if first:
        given = [pltpu.with_memory_space_constraint(a, pltpu.HBM) for a in given]
        specs = [hbm] * len(given)
        shapes = [(box + EXTRA, width)] * groups + [(width, width)] * 3 + [(size, width)] * 2
        shapes = [(s, bf16) for s in shapes] + [((EXTRA, 128), jnp.int32)]
        scratch = [pltpu.VMEM((size, width), bf16)] * 2 + [pltpu.VMEM((tiles, tile), jnp.int32)]
    else:
        specs = vmem(len(given))
        shapes = [(box, width)] * (groups - 1) + [(2 * box + EXTRA, width)]
        shapes = [(s, bf16) for s in shapes]
    small = [pltpu.with_memory_space_constraint(a, pltpu.HBM) for a in (lengths, owners)]
    return list(pl.pallas_call(
        functools.partial(attention_kernel, half, halves, groups, tile),
        in_specs=[hbm, hbm] + specs,
        out_specs=vmem(len(shapes)),
        out_shape=[jax.ShapeDtypeStruct(s, d) for s, d in shapes],
        scratch_shapes=scratch
        + [pltpu.SMEM(lengths.shape, jnp.int32), pltpu.SMEM(owners.shape, jnp.int32)]
        + [pltpu.VMEM((span, width), bf16)] * 6
        + [
            pltpu.VMEM((half_seqs * span, width), bf16),
            pltpu.VMEM((groups, EXTRA, width), jnp.float32),
            pltpu.SMEM((groups * owned + groups,), jnp.int32),
            pltpu.SemaphoreType.DMA((8 + 3 * half_seqs,)),
        ],
        compiler_params=pltpu.CompilerParams(vmem_limit_bytes=LIMIT),
        cost_estimate=pl.CostEstimate(
            flops=flops, bytes_accessed=4 * half_seqs * span * width * 2, transcendentals=0
        ),
    )(*small, *given))


def sums_of(block, boxes, exts, first, owned, tile):
    total = None
    row = lax.broadcasted_iota(jnp.int32, (ROWS_DEV, owned * tile), 0).astype(jnp.float32)
    for box, ext in zip(boxes, exts):
        slots = [ext[first + s:first + s + 1, :].astype(jnp.float32) for s in range(owned)]
        high = jnp.concatenate([r[:, 0:tile] for r in slots], axis=1)
        low = jnp.concatenate([r[:, tile:2 * tile] for r in slots], axis=1)
        key = jnp.where(high == block.astype(jnp.float32), low, -1.0)
        hot = jnp.where(row == key, 1.0, 0.0).astype(jnp.bfloat16)
        part = dot(hot, box[0:owned * tile, :])
        total = part if total is None else total + part
    return total


def live_of(exts, at):
    total = None
    for e in exts:
        row = total_of_digits(e[at:at + 1, :].astype(jnp.float32))
        total = row if total is None else total + row
    return total


def live_rows(total, like):
    width = like.shape[-1]
    row = digits_row(jnp.broadcast_to(total, (1, width)).astype(jnp.int32), width)
    return jnp.broadcast_to(row, (EXTRA, width)).astype(like.dtype)


def exts_of(boxes, base):
    return [b[base:base + EXTRA, :] for b in boxes]


def first_kernel(pairs, owned, tile, *refs):
    boxes, acc = refs[:-1], refs[-1]
    core = lax.axis_index("batch") % 2
    exts = exts_of(boxes, owned * tile)
    for side in range(2):
        for p in range(pairs):
            block = 2 * p + (1 - core if side == 0 else core)
            acc[side, p] = sums_of(block, boxes, exts, 0, owned, tile)


def side_kernel(side, pairs, owned, tile, heads, bodies, *refs):
    acc = refs[heads + bodies] if len(refs) > heads + bodies + 1 else None
    head, body, out = refs[:heads], refs[heads:heads + bodies], refs[-1]
    core = lax.axis_index("batch") % 2
    exts = exts_of(head, owned * tile)
    for p in range(pairs):
        block = 2 * p + (1 - core if side == 0 else core)
        total = sums_of(block, body, exts, owned, owned, tile)
        if acc is None:
            total = total + sums_of(block, head, exts, 0, owned, tile)
        else:
            total = total + acc[0, p]
        out[p * ROWS_DEV:(p + 1) * ROWS_DEV, :] = total.astype(out.dtype)
    if side == 0:
        out[pairs * ROWS_DEV:pairs * ROWS_DEV + EXTRA, :] = live_rows(
            live_of(exts, 2 * owned), out
        )


def pair_kernel(pairs, owned, tile, heads, *refs):
    head, own, got = refs[:heads], refs[heads], refs[heads + 1]
    outs = refs[heads + 2:]
    pair = lax.axis_index("batch") // 2
    live = live_of(exts_of(head, owned * tile), 2 * owned)
    live = live + live_of([got[pairs * ROWS_DEV:pairs * ROWS_DEV + 1, :]], 0)
    for k in range(pairs):
        at = pl.multiple_of((pair ^ k) * ROWS_DEV, ROWS_DEV)
        total = own[pl.ds(at, ROWS_DEV), :] + got[pl.ds(at, ROWS_DEV), :].astype(jnp.float32)
        outs[k][0:ROWS_DEV, :] = total.astype(outs[k].dtype)
        outs[k][ROWS_DEV:ROWS_DEV + EXTRA, :] = live_rows(live, outs[k])


def far_pair_kernel(pairs, slots, tile, *refs):
    boxes, outs = refs[:2], refs[2:]
    core, pair = lax.axis_index("batch") % 2, lax.axis_index("batch") // 2
    exts = exts_of(boxes, slots * tile)
    live = live_of(exts, slots)
    for k in range(pairs):
        block = 2 * (pair ^ k) + core
        total = sums_of(block, boxes, exts, 0, slots, tile)
        outs[k][0:ROWS_DEV, :] = total.astype(outs[k].dtype)
        outs[k][ROWS_DEV:ROWS_DEV + EXTRA, :] = live_rows(live, outs[k])


def gathered(ins):
    total = live = None
    for r in ins:
        part = r[0:ROWS_DEV, :].astype(jnp.float32)
        some = total_of_digits(r[ROWS_DEV:ROWS_DEV + 1, :].astype(jnp.float32))
        total = part if total is None else total + part
        live = some if live is None else live + some
    return total, live


def far_kernel(*refs):
    total, live = gathered(refs[:-1])
    out = refs[-1]
    out[0:ROWS_DEV, :] = total.astype(out.dtype)
    out[ROWS_DEV:ROWS_DEV + EXTRA, :] = live_rows(live, out)


def last_kernel(tokens_all, *refs):
    total, live = gathered(refs[:-1])
    refs[-1][...] = total * (tokens_all / live)


def vmem(n):
    return [pl.BlockSpec(memory_space=pltpu.VMEM)] * n


def call(kernel, shapes, flops, *args):
    return pl.pallas_call(
        kernel,
        in_specs=vmem(len(args)),
        out_specs=vmem(len(shapes)) if isinstance(shapes, list) else vmem(1)[0],
        out_shape=shapes,
        compiler_params=pltpu.CompilerParams(vmem_limit_bytes=LIMIT),
        cost_estimate=pl.CostEstimate(flops=flops, bytes_accessed=1 << 20, transcendentals=0),
    )(*args)


def on_device(groups, batches, embeds, out_grad, w_query, w_key, w_value, lengths, item_rows,
              tile_owner):
    tokens, width = embeds.shape
    halves = 2
    tile = tokens // tile_owner.shape[0]
    owned = tile_owner.shape[0] // halves // groups
    pairs = batches // 2
    rows = item_rows.reshape(-1, tile)
    f32, bf16 = jnp.float32, jnp.bfloat16
    shape = jax.ShapeDtypeStruct
    far = groups - 1
    work = 2 * pairs * ROWS_DEV * width * owned * tile

    def swap(box, k):
        return lax.ppermute(box, "group", [(i, i ^ k) for i in range(groups)])

    def across(box, k):
        return lax.ppermute(box, "batch", [(i, i ^ k) for i in range(batches)])

    near = []
    mine = attention(
        0, halves, groups, lengths, tile_owner, embeds, out_grad, w_query, w_key, w_value, rows
    )
    w_all, (emb_next, gout_next) = mine[groups:groups + 3], mine[groups + 3:groups + 5]
    counts = mine[-1]
    for half in range(halves):
        if half:
            mine = attention(
                half, halves, groups, lengths, tile_owner, emb_next, gout_next, *w_all, counts, mine[far]
            )
        near.append([mine[0]] + [swap(mine[k], k) for k in range(far - 1, 0, -1)])
    away = mine[far]

    def side(which, flops, heads, bodies, acc=None):
        out = shape((pairs * ROWS_DEV + EXTRA, width), bf16) if which == 0 else shape(
            (pairs * ROWS_DEV, width), f32)
        specs = vmem(len(heads) + len(bodies))
        args = [*heads, *bodies]
        if acc is not None:
            specs = specs + [
                pl.BlockSpec((1, pairs, ROWS_DEV, width), lambda s: (which, 0, 0, 0))
            ]
            args = args + [acc]
        return pl.pallas_call(
            functools.partial(
                side_kernel, which, pairs, owned, tile, len(heads), len(bodies)
            ),
            grid=(1,),
            in_specs=specs,
            out_specs=vmem(1)[0],
            out_shape=out,
            compiler_params=pltpu.CompilerParams(vmem_limit_bytes=LIMIT),
            cost_estimate=pl.CostEstimate(
                flops=flops, bytes_accessed=1 << 20, transcendentals=0
            ),
        )(*args)

    def plane(heads, bodies, acc=None):
        flops = work * (len(bodies) + (len(heads) if acc is None else 0))
        send = side(0, flops, heads, bodies, acc)
        got = across(send, 1)
        own = side(1, flops, heads, bodies, acc)
        parts = call(
            functools.partial(pair_kernel, pairs, owned, tile, len(heads)),
            [shape((ROWS_DEV + EXTRA, width), f32 if k == 0 else bf16) for k in range(pairs)],
            1 << 22, *heads, own, got,
        )
        return [parts[0]] + [across(parts[k], 2 * k) for k in range(1, pairs)]

    far_parts = call(
        functools.partial(far_pair_kernel, pairs, halves * owned, tile),
        [shape((ROWS_DEV + EXTRA, width), f32 if k == 0 else bf16) for k in range(pairs)],
        4 * work, away, across(away, 1),
    )
    far_parts = [far_parts[0]] + [across(far_parts[k], 2 * k) for k in range(1, pairs)]
    acc = call(
        functools.partial(first_kernel, pairs, owned, tile),
        shape((2, pairs, ROWS_DEV, width), f32), 2 * far * work, *near[0],
    )
    near_parts = plane(near[0], near[1], acc)
    far_sum = call(far_kernel, shape((ROWS_DEV + EXTRA, width), bf16), 1 << 20, *far_parts)
    return call(
        functools.partial(last_kernel, float(tokens * groups * batches)),
        shape((ROWS_DEV, width), f32), 1 << 20, *near_parts, swap(far_sum, far),
    )


def solution(mesh):
    groups, batches = mesh.shape["group"], mesh.shape["batch"]
    both = P(("group", "batch"))
    wide = P(("group", "batch"), None)

    def body(*args):
        return on_device(groups, batches, *args)

    return jax.shard_map(
        body,
        mesh=mesh,
        in_specs=(wide, wide, P(), P(), P(), both, both, both),
        out_specs=wide,
        check_vma=False,
    )
```

```python
import functools
import math

import jax
import jax.numpy as jnp
from jax import lax
from jax.experimental import pallas as pl
from jax.experimental.pallas import tpu as pltpu
from jax.sharding import PartitionSpec as P


HEADS = 2
ROWS_DEV = 256
EXTRA = 8
BASE = 128
LIMIT = 24 << 20
NT = (((1,), (1,)), ((), ()))
TN = (((0,), (0,)), ((), ()))


def dot(a, b, dims=(((1,), (0,)), ((), ()))):
    return lax.dot_general(a, b, dims, preferred_element_type=jnp.float32)


def digits_row(total, width):
    lane = lax.broadcasted_iota(jnp.int32, (1, width), 1)
    low, mid, high = total % BASE, (total // BASE) % BASE, total // (BASE * BASE)
    row = jnp.where(lane == 0, low, jnp.where(lane == 1, mid, jnp.where(lane == 2, high, 0)))
    return row.astype(jnp.float32)


def total_of_digits(row):
    return row[:, 0:1] + row[:, 1:2] * float(BASE) + row[:, 2:3] * float(BASE * BASE)


def attention_kernel(half, halves, groups, tile, len_h, own_h, *refs):
    first = half == 0
    if first:
        (emb_h, gout_h, wq_h, wk_h, wv_h, rows_h), refs = refs[:6], refs[6:]
        outs, refs = refs[:groups], refs[groups:]
        (wq, wk, wv, emb_next, gout_next, counts), refs = refs[:6], refs[6:]
        (emb, gout, rows), refs = refs[:3], refs[3:]
    else:
        (emb, gout, wq, wk, wv, counts, kept), refs = refs[:7], refs[7:]
        outs, refs = refs[:groups], refs[groups:]
    len_ref, own_ref, q_s, k_s, v_s, dq_s, dk_s, dv_s, tok_s, ext_s, idx_s, sems = refs
    width = emb.shape[1]
    half_seqs = len_ref.shape[0] // halves
    half_tiles = own_ref.shape[0] // halves
    owned = half_tiles // groups
    size = emb.shape[0]
    span = size // half_seqs
    head = width // HEADS
    scale = 1.0 / math.sqrt(head)
    block = span // 2
    sub = block // 2

    def load(source, target, sem):
        return pltpu.make_async_copy(source, target, sem)

    def load_rows(source, target, base, at, count, sem):
        return load(source.at[pl.ds(base + at, count)], target.at[pl.ds(at, count)], sem)

    wait_len, wait_own = load(len_h, len_ref, sems.at[0]), load(own_h, own_ref, sems.at[1])
    if first:
        wait_len.start()
        head_loads = [load(wq_h, wq, sems.at[2]), load(wk_h, wk, sems.at[3])]
        head_loads += [load(wv_h, wv, sems.at[4])]
        wait_rows = load(rows_h, rows, sems.at[5])

        def loads(s):
            low = load_rows(emb_h, emb, 0, s * span, block, sems.at[8 + 3 * s])
            high = load_rows(emb_h, emb, 0, s * span + block, block, sems.at[9 + 3 * s])
            other = load_rows(gout_h, gout, 0, s * span, span, sems.at[10 + 3 * s])
            return low, high, other

        for s in range(half_seqs):
            low, high, other = loads(s)
            low.start()
            if s == 0:
                for c in head_loads:
                    c.start()
            high.start()
            other.start()
        wait_rows.start()
        later = [
            load_rows(emb_h, emb_next, size, 0, size, sems.at[6]),
            load_rows(gout_h, gout_next, size, 0, size, sems.at[7]),
        ]
    wait_own.start()

    def gate(raw, grad, weight):
        grown = jnp.exp2(raw * (-scale * math.log2(math.e)))
        sigma = 1.0 / (1.0 + grown)
        act = raw * scale * sigma
        slope = sigma + act * (1.0 - sigma)
        return (
            (act * weight).astype(jnp.bfloat16),
            (grad * weight * slope).astype(jnp.bfloat16),
        )

    def project(base, at):
        rows_in = emb[pl.ds(base + at, block), :]
        q_s[at:at + block, :] = dot(rows_in, wq[...]).astype(jnp.bfloat16)
        k_s[at:at + block, :] = dot(rows_in, wk[...]).astype(jnp.bfloat16)
        v_s[at:at + block, :] = dot(rows_in, wv[...]).astype(jnp.bfloat16)

    def run(base, count, live):
        if live > block:
            project(base, block)
        lane = lax.broadcasted_iota(jnp.int32, (1, block), 1)
        inverse = 1.0 / jnp.broadcast_to(count, (1, block)).astype(jnp.float32)
        causal = lax.broadcasted_iota(jnp.int32, (sub, sub), 0) <= lax.broadcasted_iota(
            jnp.int32, (sub, sub), 1
        )
        zeros = jnp.zeros((sub, sub), jnp.bfloat16)
        for h in range(HEADS):
            cols = slice(h * head, (h + 1) * head)
            att, sco = {}, {}
            for i in range(live // block):
                weight = jnp.where(lane + i * block < count, inverse, 0.0)
                iq = q_s[i * block:(i + 1) * block, cols]
                ig = gout[pl.ds(base + i * block, block), cols]
                for j in range(i + 1):
                    jk = k_s[j * block:(j + 1) * block, cols]
                    jv = v_s[j * block:(j + 1) * block, cols]
                    raw = dot(jk, iq, NT)
                    grad = dot(jv, ig, NT)
                    if i != j:
                        att[j, i], sco[j, i] = gate(raw, grad, weight)
                        continue
                    low, high = weight[:, :sub], weight[:, sub:]
                    a0, s0 = gate(
                        raw[:sub, :sub], grad[:sub, :sub], jnp.where(causal, low, 0.0)
                    )
                    a1, s1 = gate(raw[:sub, sub:], grad[:sub, sub:], high)
                    a2, s2 = gate(
                        raw[sub:, sub:], grad[sub:, sub:], jnp.where(causal, high, 0.0)
                    )

                    def whole(x, y, z):
                        return jnp.concatenate(
                            [
                                jnp.concatenate([x, y], axis=1),
                                jnp.concatenate([zeros, z], axis=1),
                            ],
                            axis=0,
                        )

                    att[j, i], sco[j, i] = whole(a0, a1, a2), whole(s0, s1, s2)
            for j in range(live // block):
                vg = kg = None
                for i in range(j, live // block):
                    iq = q_s[i * block:(i + 1) * block, cols]
                    ig = gout[pl.ds(base + i * block, block), cols]
                    a, b = dot(att[j, i], ig), dot(sco[j, i], iq)
                    vg = a if vg is None else vg + a
                    kg = b if kg is None else kg + b
                dv_s[j * block:(j + 1) * block, cols] = vg.astype(jnp.bfloat16)
                dk_s[j * block:(j + 1) * block, cols] = (kg * scale).astype(jnp.bfloat16)
            for i in range(live // block):
                qg = None
                for j in range(i + 1):
                    jk = k_s[j * block:(j + 1) * block, cols]
                    c = dot(sco[j, i], jk, TN)
                    qg = c if qg is None else qg + c
                dq_s[i * block:(i + 1) * block, cols] = (qg * scale).astype(jnp.bfloat16)
        token = dot(dq_s[0:live, :], wq[...], NT)
        token = token + dot(dk_s[0:live, :], wk[...], NT)
        token = token + dot(dv_s[0:live, :], wv[...], NT)
        tok_s[pl.ds(base, live), :] = token.astype(jnp.bfloat16)
        if live < span:
            tok_s[pl.ds(base + live, span - live), :] = jnp.zeros((span - live, width), jnp.bfloat16)

    if first:
        for c in head_loads:
            c.wait()
        wait_len.wait()
        for s in range(len_ref.shape[0]):
            counts[s:s + 1, :] = jnp.broadcast_to(len_ref[s], (1, counts.shape[1]))

    def one(s, carry):
        base = pl.multiple_of(s * span, span)
        if first:
            low, high, other = loads(s)
            low.wait()
        project(base, 0)
        if first:
            high.wait()
            other.wait()

            @pl.when(s == half_seqs - 1)
            def _():
                for c in later:
                    c.start()

        if first:
            count = len_ref[half * half_seqs + s]
        else:
            count = jnp.max(counts[pl.ds(half * half_seqs + s, 1), :])
        if first:
            pl.when(count <= block)(functools.partial(run, base, count, block))
            pl.when(count > block)(functools.partial(run, base, count, span))
        else:
            run(base, count, span)
        return carry

    lax.fori_loop(0, half_seqs, one, 0)
    wait_own.wait()

    me = lax.axis_index("group")

    def place(part):
        for g in range(groups):
            idx_s[groups * owned + g] = 0
        for t in range(half_tiles):
            owner = own_ref[part * half_tiles + t]
            seen = idx_s[groups * owned + owner]
            idx_s[owner * owned + seen] = t
            idx_s[groups * owned + owner] = seen + 1

    if first:
        wait_rows.wait()
        total = len_ref[0]
        for s in range(1, len_ref.shape[0]):
            total = total + len_ref[s]
        for k in range(groups):
            ext_s[k] = jnp.zeros(ext_s.shape[1:], jnp.float32)
            ext_s[k, halves * owned:halves * owned + 1, :] = digits_row(total, width)
        for part in range(halves - 1, -1, -1):
            place(part)
            for k in range(groups):
                owner = me ^ k
                for s in range(owned):
                    t = idx_s[owner * owned + s] + part * half_tiles
                    row = rows[pl.ds(t, 1), :]
                    at = part * owned + s
                    ext_s[k, at:at + 1, 0:tile] = (row // ROWS_DEV).astype(jnp.float32)
                    ext_s[k, at:at + 1, tile:2 * tile] = (row % ROWS_DEV).astype(jnp.float32)
        for k in range(groups):
            outs[k][owned * tile:owned * tile + EXTRA, :] = ext_s[k].astype(jnp.bfloat16)
    else:
        place(half)
    for k in range(groups):
        owner = me ^ k
        shift = 0
        if not first and k == groups - 1:
            shift = owned * tile
            outs[k][0:shift, :] = kept[0:shift, :]
            outs[k][2 * shift:2 * shift + EXTRA, :] = kept[shift:shift + EXTRA, :]
        for s in range(owned):
            t = idx_s[owner * owned + s]
            outs[k][shift + s * tile:shift + (s + 1) * tile, :] = tok_s[
                pl.ds(pl.multiple_of(t * tile, tile), tile), :
            ]
    if first:
        for c in later:
            c.wait()


def attention(half, halves, groups, lengths, owners, *given):
    width = given[0].shape[1]
    first = half == 0
    size = given[0].shape[0] // (halves if first else 1)
    seqs, tiles = lengths.shape[0], owners.shape[0]
    span = size * halves // seqs
    tile = size * halves // tiles
    half_seqs, half_tiles = seqs // halves, tiles // halves
    owned = half_tiles // groups
    bf16 = jnp.bfloat16
    box = owned * tile
    flops = half_seqs * (2 * span * width * width * 6 + 10 * span * span * width)
    hbm = pl.BlockSpec(memory_space=pltpu.HBM)
    scratch = []
    if first:
        given = [pltpu.with_memory_space_constraint(a, pltpu.HBM) for a in given]
        specs = [hbm] * len(given)
        shapes = [(box + EXTRA, width)] * groups + [(width, width)] * 3 + [(size, width)] * 2
        shapes = [(s, bf16) for s in shapes] + [((EXTRA, 128), jnp.int32)]
        scratch = [pltpu.VMEM((size, width), bf16)] * 2 + [pltpu.VMEM((tiles, tile), jnp.int32)]
    else:
        specs = vmem(len(given))
        shapes = [(box, width)] * (groups - 1) + [(2 * box + EXTRA, width)]
        shapes = [(s, bf16) for s in shapes]
    small = [pltpu.with_memory_space_constraint(a, pltpu.HBM) for a in (lengths, owners)]
    return list(pl.pallas_call(
        functools.partial(attention_kernel, half, halves, groups, tile),
        in_specs=[hbm, hbm] + specs,
        out_specs=vmem(len(shapes)),
        out_shape=[jax.ShapeDtypeStruct(s, d) for s, d in shapes],
        scratch_shapes=scratch
        + [pltpu.SMEM(lengths.shape, jnp.int32), pltpu.SMEM(owners.shape, jnp.int32)]
        + [pltpu.VMEM((span, width), bf16)] * 6
        + [
            pltpu.VMEM((half_seqs * span, width), bf16),
            pltpu.VMEM((groups, EXTRA, width), jnp.float32),
            pltpu.SMEM((groups * owned + groups,), jnp.int32),
            pltpu.SemaphoreType.DMA((8 + 3 * half_seqs,)),
        ],
        compiler_params=pltpu.CompilerParams(vmem_limit_bytes=LIMIT),
        cost_estimate=pl.CostEstimate(
            flops=flops, bytes_accessed=4 * half_seqs * span * width * 2, transcendentals=0
        ),
    )(*small, *given))


def sums_of(block, boxes, exts, first, owned, tile):
    total = None
    row = lax.broadcasted_iota(jnp.int32, (ROWS_DEV, owned * tile), 0).astype(jnp.float32)
    for box, ext in zip(boxes, exts):
        slots = [ext[first + s:first + s + 1, :].astype(jnp.float32) for s in range(owned)]
        high = jnp.concatenate([r[:, 0:tile] for r in slots], axis=1)
        low = jnp.concatenate([r[:, tile:2 * tile] for r in slots], axis=1)
        key = jnp.where(high == block.astype(jnp.float32), low, -1.0)
        hot = jnp.where(row == key, 1.0, 0.0).astype(jnp.bfloat16)
        part = dot(hot, box[0:owned * tile, :])
        total = part if total is None else total + part
    return total


def live_of(exts, at):
    total = None
    for e in exts:
        row = total_of_digits(e[at:at + 1, :].astype(jnp.float32))
        total = row if total is None else total + row
    return total


def live_rows(total, like):
    width = like.shape[-1]
    row = digits_row(jnp.broadcast_to(total, (1, width)).astype(jnp.int32), width)
    return jnp.broadcast_to(row, (EXTRA, width)).astype(like.dtype)


def exts_of(boxes, base):
    return [b[base:base + EXTRA, :] for b in boxes]


def early_kernel(side, pairs, owned, tile, heads, *refs):
    head, later, out = refs[:heads], refs[heads], refs[-1]
    core = lax.axis_index("batch") % 2
    exts = exts_of(head, owned * tile)
    for p in range(pairs):
        block = 2 * p + (1 - core if side == 0 else core)
        total = sums_of(block, head, exts, 0, owned, tile)
        total = total + sums_of(block, [later], exts[:1], owned, owned, tile)
        out[p * ROWS_DEV:(p + 1) * ROWS_DEV, :] = total.astype(out.dtype)
    if side == 0:
        base = pairs * ROWS_DEV
        out[base:base + EXTRA, :] = live_rows(live_of(exts, 2 * owned), out)
        for n in range(1, heads):
            out[base + n * EXTRA:base + (n + 1) * EXTRA, :] = exts[n]


def near_pair_kernel(pairs, owned, tile, heads, *refs):
    head, refs = refs[:heads], refs[heads:]
    own, got, refs = refs[0], refs[1], refs[2:]
    late, outs = refs[:2 * (heads - 1)], refs[2 * (heads - 1):]
    core, pair = lax.axis_index("batch") % 2, lax.axis_index("batch") // 2
    exts = exts_of(head, owned * tile)
    base = pairs * ROWS_DEV
    live = live_of(exts, 2 * owned) + live_of([got[base:base + 1, :]], 0)
    exts = exts[1:] + [
        got[base + n * EXTRA:base + (n + 1) * EXTRA, :] for n in range(1, heads)
    ]
    for k in range(pairs):
        at = pl.multiple_of((pair ^ k) * ROWS_DEV, ROWS_DEV)
        total = own[pl.ds(at, ROWS_DEV), :] + got[pl.ds(at, ROWS_DEV), :].astype(jnp.float32)
        total = total + sums_of(2 * (pair ^ k) + core, late, exts, owned, owned, tile)
        outs[k][0:ROWS_DEV, :] = total.astype(outs[k].dtype)
        outs[k][ROWS_DEV:ROWS_DEV + EXTRA, :] = live_rows(live, outs[k])


def far_pair_kernel(pairs, slots, tile, *refs):
    boxes, outs = refs[:2], refs[2:]
    core, pair = lax.axis_index("batch") % 2, lax.axis_index("batch") // 2
    exts = exts_of(boxes, slots * tile)
    live = live_of(exts, slots)
    for k in range(pairs):
        block = 2 * (pair ^ k) + core
        total = sums_of(block, boxes, exts, 0, slots, tile)
        outs[k][0:ROWS_DEV, :] = total.astype(outs[k].dtype)
        outs[k][ROWS_DEV:ROWS_DEV + EXTRA, :] = live_rows(live, outs[k])


def gathered(ins):
    total = live = None
    for r in ins:
        part = r[0:ROWS_DEV, :].astype(jnp.float32)
        some = total_of_digits(r[ROWS_DEV:ROWS_DEV + 1, :].astype(jnp.float32))
        total = part if total is None else total + part
        live = some if live is None else live + some
    return total, live


def far_kernel(*refs):
    total, live = gathered(refs[:-1])
    out = refs[-1]
    out[0:ROWS_DEV, :] = total.astype(out.dtype)
    out[ROWS_DEV:ROWS_DEV + EXTRA, :] = live_rows(live, out)


def last_kernel(tokens_all, *refs):
    total, live = gathered(refs[:-1])
    refs[-1][...] = total * (tokens_all / live)


def vmem(n):
    return [pl.BlockSpec(memory_space=pltpu.VMEM)] * n


def call(kernel, shapes, flops, *args):
    return pl.pallas_call(
        kernel,
        in_specs=vmem(len(args)),
        out_specs=vmem(len(shapes)) if isinstance(shapes, list) else vmem(1)[0],
        out_shape=shapes,
        compiler_params=pltpu.CompilerParams(vmem_limit_bytes=LIMIT),
        cost_estimate=pl.CostEstimate(flops=flops, bytes_accessed=1 << 20, transcendentals=0),
    )(*args)


def on_device(groups, batches, embeds, out_grad, w_query, w_key, w_value, lengths, item_rows,
              tile_owner):
    tokens, width = embeds.shape
    halves = 2
    tile = tokens // tile_owner.shape[0]
    owned = tile_owner.shape[0] // halves // groups
    pairs = batches // 2
    rows = item_rows.reshape(-1, tile)
    f32, bf16 = jnp.float32, jnp.bfloat16
    shape = jax.ShapeDtypeStruct
    far = groups - 1
    work = 2 * pairs * ROWS_DEV * width * owned * tile

    def swap(box, k):
        return lax.ppermute(box, "group", [(i, i ^ k) for i in range(groups)])

    def across(box, k):
        return lax.ppermute(box, "batch", [(i, i ^ k) for i in range(batches)])

    near = []
    mine = attention(
        0, halves, groups, lengths, tile_owner, embeds, out_grad, w_query, w_key, w_value, rows
    )
    w_all, (emb_next, gout_next) = mine[groups:groups + 3], mine[groups + 3:groups + 5]
    counts = mine[-1]
    for half in range(halves):
        if half:
            mine = attention(
                half, halves, groups, lengths, tile_owner, emb_next, gout_next, *w_all, counts, mine[far]
            )
        near.append([mine[0]] + [swap(mine[k], k) for k in range(far - 1, 0, -1)])
    away = mine[far]

    def parts_of(kernel, flops, *args):
        return call(
            kernel, [shape((ROWS_DEV + EXTRA, width), f32 if k == 0 else bf16) for k in range(pairs)],
            flops, *args,
        )

    far_parts = parts_of(
        functools.partial(far_pair_kernel, pairs, halves * owned, tile),
        4 * work, away, across(away, 1),
    )
    far_parts = [far_parts[0]] + [across(far_parts[k], 2 * k) for k in range(pairs - 1, 0, -1)]
    tall = pairs * ROWS_DEV
    send, own = [
        call(
            functools.partial(early_kernel, which, pairs, owned, tile, far),
            shape((rows_out, width), kind), (far + 1) * work, *near[0], near[1][0],
        )
        for which, rows_out, kind in ((0, tall + far * EXTRA, bf16), (1, tall, f32))
    ]
    got = across(send, 1)
    late = near[1][1:]
    near_parts = parts_of(
        functools.partial(near_pair_kernel, pairs, owned, tile, far),
        4 * work, *near[0], own, got, *late,
        *[across(box, 1) for box in late],
    )
    near_parts = [near_parts[0]] + [across(near_parts[k], 2 * k) for k in range(pairs - 1, 0, -1)]
    far_sum = call(far_kernel, shape((ROWS_DEV + EXTRA, width), bf16), 1 << 20, *far_parts)
    return call(
        functools.partial(last_kernel, float(tokens * groups * batches)),
        shape((ROWS_DEV, width), f32), 1 << 20, *near_parts, swap(far_sum, far),
    )


def solution(mesh):
    groups, batches = mesh.shape["group"], mesh.shape["batch"]
    both = P(("group", "batch"))
    wide = P(("group", "batch"), None)

    def body(*args):
        return on_device(groups, batches, *args)

    return jax.shard_map(
        body,
        mesh=mesh,
        in_specs=(wide, wide, P(), P(), P(), both, both, both),
        out_specs=wide,
        check_vma=False,
    )
```

```python
import functools
import math

import jax
import jax.numpy as jnp
from jax import lax
from jax.experimental import pallas as pl
from jax.experimental.pallas import tpu as pltpu
from jax.sharding import PartitionSpec as P


HEADS = 2
ROWS_DEV = 256
EXTRA = 8
BASE = 128
LIMIT = 24 << 20
NT = (((1,), (1,)), ((), ()))
TN = (((0,), (0,)), ((), ()))


def dot(a, b, dims=(((1,), (0,)), ((), ()))):
    return lax.dot_general(a, b, dims, preferred_element_type=jnp.float32)


def digits_row(total, width):
    lane = lax.broadcasted_iota(jnp.int32, (1, width), 1)
    low, mid, high = total % BASE, (total // BASE) % BASE, total // (BASE * BASE)
    row = jnp.where(lane == 0, low, jnp.where(lane == 1, mid, jnp.where(lane == 2, high, 0)))
    return row.astype(jnp.float32)


def total_of_digits(row):
    return row[:, 0:1] + row[:, 1:2] * float(BASE) + row[:, 2:3] * float(BASE * BASE)


def attention_kernel(half, halves, groups, tile, len_h, own_h, *refs):
    first = half == 0
    if first:
        (emb_h, gout_h, wq_h, wk_h, wv_h, rows_h), refs = refs[:6], refs[6:]
        outs, refs = refs[:groups], refs[groups:]
        (wq, wk, wv, emb_next, gout_next, counts), refs = refs[:6], refs[6:]
        (emb, gout, rows), refs = refs[:3], refs[3:]
    else:
        (emb, gout, wq, wk, wv, counts, kept), refs = refs[:7], refs[7:]
        outs, refs = refs[:groups], refs[groups:]
    len_ref, own_ref, q_s, k_s, v_s, dq_s, dk_s, dv_s, tok_s, ext_s, idx_s, sems = refs
    width = emb.shape[1]
    half_seqs = len_ref.shape[0] // halves
    half_tiles = own_ref.shape[0] // halves
    owned = half_tiles // groups
    size = emb.shape[0]
    span = size // half_seqs
    head = width // HEADS
    scale = 1.0 / math.sqrt(head)
    block = span // 2
    sub = block // 2

    def load(source, target, sem):
        return pltpu.make_async_copy(source, target, sem)

    def load_rows(source, target, base, at, count, sem):
        return load(source.at[pl.ds(base + at, count)], target.at[pl.ds(at, count)], sem)

    wait_len, wait_own = load(len_h, len_ref, sems.at[0]), load(own_h, own_ref, sems.at[1])
    if first:
        wait_len.start()
        head_loads = [load(wq_h, wq, sems.at[2]), load(wk_h, wk, sems.at[3])]
        head_loads += [load(wv_h, wv, sems.at[4])]
        wait_rows = load(rows_h, rows, sems.at[5])

        def loads(s):
            low = load_rows(emb_h, emb, 0, s * span, block, sems.at[8 + 3 * s])
            high = load_rows(emb_h, emb, 0, s * span + block, block, sems.at[9 + 3 * s])
            other = load_rows(gout_h, gout, 0, s * span, span, sems.at[10 + 3 * s])
            return low, high, other

        for s in range(half_seqs):
            low, high, other = loads(s)
            low.start()
            if s == 0:
                for c in head_loads:
                    c.start()
            high.start()
            other.start()
        wait_rows.start()
        later = [
            load_rows(emb_h, emb_next, size, 0, size, sems.at[6]),
            load_rows(gout_h, gout_next, size, 0, size, sems.at[7]),
        ]
    wait_own.start()

    def gate(raw, grad, weight):
        grown = jnp.exp2(raw * (-scale * math.log2(math.e)))
        sigma = 1.0 / (1.0 + grown)
        act = raw * scale * sigma
        slope = sigma + act * (1.0 - sigma)
        return (
            (act * weight).astype(jnp.bfloat16),
            (grad * weight * slope).astype(jnp.bfloat16),
        )

    def project(base, at):
        rows_in = emb[pl.ds(base + at, block), :]
        q_s[at:at + block, :] = dot(rows_in, wq[...]).astype(jnp.bfloat16)
        k_s[at:at + block, :] = dot(rows_in, wk[...]).astype(jnp.bfloat16)
        v_s[at:at + block, :] = dot(rows_in, wv[...]).astype(jnp.bfloat16)

    def run(base, count, live):
        if live > block:
            project(base, block)
        lane = lax.broadcasted_iota(jnp.int32, (1, block), 1)
        inverse = 1.0 / jnp.broadcast_to(count, (1, block)).astype(jnp.float32)
        causal = lax.broadcasted_iota(jnp.int32, (sub, sub), 0) <= lax.broadcasted_iota(
            jnp.int32, (sub, sub), 1
        )
        zeros = jnp.zeros((sub, sub), jnp.bfloat16)
        for h in range(HEADS):
            cols = slice(h * head, (h + 1) * head)
            att, sco = {}, {}
            for i in range(live // block):
                weight = jnp.where(lane + i * block < count, inverse, 0.0)
                iq = q_s[i * block:(i + 1) * block, cols]
                ig = gout[pl.ds(base + i * block, block), cols]
                for j in range(i + 1):
                    jk = k_s[j * block:(j + 1) * block, cols]
                    jv = v_s[j * block:(j + 1) * block, cols]
                    raw = dot(jk, iq, NT)
                    grad = dot(jv, ig, NT)
                    if i != j:
                        att[j, i], sco[j, i] = gate(raw, grad, weight)
                        continue
                    low, high = weight[:, :sub], weight[:, sub:]
                    a0, s0 = gate(
                        raw[:sub, :sub], grad[:sub, :sub], jnp.where(causal, low, 0.0)
                    )
                    a1, s1 = gate(raw[:sub, sub:], grad[:sub, sub:], high)
                    a2, s2 = gate(
                        raw[sub:, sub:], grad[sub:, sub:], jnp.where(causal, high, 0.0)
                    )

                    def whole(x, y, z):
                        return jnp.concatenate(
                            [
                                jnp.concatenate([x, y], axis=1),
                                jnp.concatenate([zeros, z], axis=1),
                            ],
                            axis=0,
                        )

                    att[j, i], sco[j, i] = whole(a0, a1, a2), whole(s0, s1, s2)
            for j in range(live // block):
                vg = kg = None
                for i in range(j, live // block):
                    iq = q_s[i * block:(i + 1) * block, cols]
                    ig = gout[pl.ds(base + i * block, block), cols]
                    a, b = dot(att[j, i], ig), dot(sco[j, i], iq)
                    vg = a if vg is None else vg + a
                    kg = b if kg is None else kg + b
                dv_s[j * block:(j + 1) * block, cols] = vg.astype(jnp.bfloat16)
                dk_s[j * block:(j + 1) * block, cols] = (kg * scale).astype(jnp.bfloat16)
            for i in range(live // block):
                qg = None
                for j in range(i + 1):
                    jk = k_s[j * block:(j + 1) * block, cols]
                    c = dot(sco[j, i], jk, TN)
                    qg = c if qg is None else qg + c
                dq_s[i * block:(i + 1) * block, cols] = (qg * scale).astype(jnp.bfloat16)
        token = dot(dq_s[0:live, :], wq[...], NT)
        token = token + dot(dk_s[0:live, :], wk[...], NT)
        token = token + dot(dv_s[0:live, :], wv[...], NT)
        tok_s[pl.ds(base, live), :] = token.astype(jnp.bfloat16)
        if live < span:
            tok_s[pl.ds(base + live, span - live), :] = jnp.zeros((span - live, width), jnp.bfloat16)

    if first:
        for c in head_loads:
            c.wait()
        wait_len.wait()
        for s in range(len_ref.shape[0]):
            counts[s:s + 1, :] = jnp.broadcast_to(len_ref[s], (1, counts.shape[1]))

    def one(s, carry):
        base = pl.multiple_of(s * span, span)
        if first:
            low, high, other = loads(s)
            low.wait()
        project(base, 0)
        if first:
            high.wait()
            other.wait()

            @pl.when(s == half_seqs - 1)
            def _():
                for c in later:
                    c.start()

        if first:
            count = len_ref[half * half_seqs + s]
        else:
            count = jnp.max(counts[pl.ds(half * half_seqs + s, 1), :])
        if first:
            pl.when(count <= block)(functools.partial(run, base, count, block))
            pl.when(count > block)(functools.partial(run, base, count, span))
        else:
            run(base, count, span)
        return carry

    lax.fori_loop(0, half_seqs, one, 0)
    wait_own.wait()

    me = lax.axis_index("group")

    def place(part):
        for g in range(groups):
            idx_s[groups * owned + g] = 0
        for t in range(half_tiles):
            owner = own_ref[part * half_tiles + t]
            seen = idx_s[groups * owned + owner]
            idx_s[owner * owned + seen] = t
            idx_s[groups * owned + owner] = seen + 1

    if first:
        wait_rows.wait()
        total = len_ref[0]
        for s in range(1, len_ref.shape[0]):
            total = total + len_ref[s]
        for k in range(groups):
            ext_s[k] = jnp.zeros(ext_s.shape[1:], jnp.float32)
            ext_s[k, halves * owned:halves * owned + 1, :] = digits_row(total, width)
        for part in range(halves - 1, -1, -1):
            place(part)
            for k in range(groups):
                owner = me ^ k
                for s in range(owned):
                    t = idx_s[owner * owned + s] + part * half_tiles
                    row = rows[pl.ds(t, 1), :]
                    at = part * owned + s
                    ext_s[k, at:at + 1, 0:tile] = (row // ROWS_DEV).astype(jnp.float32)
                    ext_s[k, at:at + 1, tile:2 * tile] = (row % ROWS_DEV).astype(jnp.float32)
        for k in range(groups):
            outs[k][owned * tile:owned * tile + EXTRA, :] = ext_s[k].astype(jnp.bfloat16)
    else:
        place(half)
    for k in range(groups):
        owner = me ^ k
        shift = 0
        if not first and k == groups - 1:
            shift = owned * tile
            outs[k][0:shift, :] = kept[0:shift, :]
            outs[k][2 * shift:2 * shift + EXTRA, :] = kept[shift:shift + EXTRA, :]
        for s in range(owned):
            t = idx_s[owner * owned + s]
            outs[k][shift + s * tile:shift + (s + 1) * tile, :] = tok_s[
                pl.ds(pl.multiple_of(t * tile, tile), tile), :
            ]
    if first:
        for c in later:
            c.wait()


def attention(half, halves, groups, lengths, owners, *given):
    width = given[0].shape[1]
    first = half == 0
    size = given[0].shape[0] // (halves if first else 1)
    seqs, tiles = lengths.shape[0], owners.shape[0]
    span = size * halves // seqs
    tile = size * halves // tiles
    half_seqs, half_tiles = seqs // halves, tiles // halves
    owned = half_tiles // groups
    bf16 = jnp.bfloat16
    box = owned * tile
    flops = half_seqs * (2 * span * width * width * 6 + 10 * span * span * width)
    hbm = pl.BlockSpec(memory_space=pltpu.HBM)
    scratch = []
    if first:
        given = [pltpu.with_memory_space_constraint(a, pltpu.HBM) for a in given]
        specs = [hbm] * len(given)
        shapes = [(box + EXTRA, width)] * groups + [(width, width)] * 3 + [(size, width)] * 2
        shapes = [(s, bf16) for s in shapes] + [((EXTRA, 128), jnp.int32)]
        scratch = [pltpu.VMEM((size, width), bf16)] * 2 + [pltpu.VMEM((tiles, tile), jnp.int32)]
    else:
        specs = vmem(len(given))
        shapes = [(box, width)] * (groups - 1) + [(2 * box + EXTRA, width)]
        shapes = [(s, bf16) for s in shapes]
    small = [pltpu.with_memory_space_constraint(a, pltpu.HBM) for a in (lengths, owners)]
    return list(pl.pallas_call(
        functools.partial(attention_kernel, half, halves, groups, tile),
        in_specs=[hbm, hbm] + specs,
        out_specs=vmem(len(shapes)),
        out_shape=[jax.ShapeDtypeStruct(s, d) for s, d in shapes],
        scratch_shapes=scratch
        + [pltpu.SMEM(lengths.shape, jnp.int32), pltpu.SMEM(owners.shape, jnp.int32)]
        + [pltpu.VMEM((span, width), bf16)] * 6
        + [
            pltpu.VMEM((half_seqs * span, width), bf16),
            pltpu.VMEM((groups, EXTRA, width), jnp.float32),
            pltpu.SMEM((groups * owned + groups,), jnp.int32),
            pltpu.SemaphoreType.DMA((8 + 3 * half_seqs,)),
        ],
        compiler_params=pltpu.CompilerParams(vmem_limit_bytes=LIMIT),
        cost_estimate=pl.CostEstimate(
            flops=flops, bytes_accessed=4 * half_seqs * span * width * 2, transcendentals=0
        ),
    )(*small, *given))


def sums_of(block, boxes, exts, first, owned, tile):
    total = None
    row = lax.broadcasted_iota(jnp.int32, (ROWS_DEV, owned * tile), 0).astype(jnp.float32)
    for box, ext in zip(boxes, exts):
        slots = [ext[first + s:first + s + 1, :].astype(jnp.float32) for s in range(owned)]
        high = jnp.concatenate([r[:, 0:tile] for r in slots], axis=1)
        low = jnp.concatenate([r[:, tile:2 * tile] for r in slots], axis=1)
        key = jnp.where(high == block.astype(jnp.float32), low, -1.0)
        hot = jnp.where(row == key, 1.0, 0.0).astype(jnp.bfloat16)
        part = dot(hot, box[0:owned * tile, :])
        total = part if total is None else total + part
    return total


def live_of(exts, at):
    total = None
    for e in exts:
        row = total_of_digits(e[at:at + 1, :].astype(jnp.float32))
        total = row if total is None else total + row
    return total


def live_rows(total, like):
    width = like.shape[-1]
    row = digits_row(jnp.broadcast_to(total, (1, width)).astype(jnp.int32), width)
    return jnp.broadcast_to(row, (EXTRA, width)).astype(like.dtype)


def exts_of(boxes, base):
    return [b[base:base + EXTRA, :] for b in boxes]


def early_kernel(side, pairs, owned, tile, heads, *refs):
    head, later, out = refs[:heads], refs[heads], refs[-1]
    core = lax.axis_index("batch") % 2
    exts = exts_of(head, owned * tile)
    for p in range(pairs):
        block = 2 * p + (1 - core if side == 0 else core)
        total = sums_of(block, head, exts, 0, owned, tile)
        total = total + sums_of(block, [later], exts[:1], owned, owned, tile)
        out[p * ROWS_DEV:(p + 1) * ROWS_DEV, :] = total.astype(out.dtype)
    if side == 0:
        base = pairs * ROWS_DEV
        out[base:base + EXTRA, :] = live_rows(live_of(exts, 2 * owned), out)
        for n in range(1, heads):
            out[base + n * EXTRA:base + (n + 1) * EXTRA, :] = exts[n]


def near_pair_kernel(pairs, owned, tile, heads, *refs):
    head, refs = refs[:heads], refs[heads:]
    own, got, refs = refs[0], refs[1], refs[2:]
    late, outs = refs[:2 * (heads - 1)], refs[2 * (heads - 1):]
    core, pair = lax.axis_index("batch") % 2, lax.axis_index("batch") // 2
    exts = exts_of(head, owned * tile)
    base = pairs * ROWS_DEV
    live = live_of(exts, 2 * owned) + live_of([got[base:base + 1, :]], 0)
    exts = exts[1:] + [
        got[base + n * EXTRA:base + (n + 1) * EXTRA, :] for n in range(1, heads)
    ]
    for k in range(pairs):
        at = pl.multiple_of((pair ^ k) * ROWS_DEV, ROWS_DEV)
        total = own[pl.ds(at, ROWS_DEV), :] + got[pl.ds(at, ROWS_DEV), :].astype(jnp.float32)
        total = total + sums_of(2 * (pair ^ k) + core, late, exts, owned, owned, tile)
        outs[k][0:ROWS_DEV, :] = total.astype(outs[k].dtype)
        outs[k][ROWS_DEV:ROWS_DEV + EXTRA, :] = live_rows(live, outs[k])


def far_pair_kernel(pairs, slots, tile, *refs):
    boxes, outs = refs[:2], refs[2:]
    core, pair = lax.axis_index("batch") % 2, lax.axis_index("batch") // 2
    exts = exts_of(boxes, slots * tile)
    live = live_of(exts, slots)
    for k in range(pairs):
        block = 2 * (pair ^ k) + core
        total = sums_of(block, boxes, exts, 0, slots, tile)
        outs[k][0:ROWS_DEV, :] = total.astype(outs[k].dtype)
        outs[k][ROWS_DEV:ROWS_DEV + EXTRA, :] = live_rows(live, outs[k])


def gathered(ins):
    total = live = None
    for r in ins:
        part = r[0:ROWS_DEV, :].astype(jnp.float32)
        some = total_of_digits(r[ROWS_DEV:ROWS_DEV + 1, :].astype(jnp.float32))
        total = part if total is None else total + part
        live = some if live is None else live + some
    return total, live


def far_kernel(*refs):
    total, live = gathered(refs[:-1])
    out = refs[-1]
    out[0:ROWS_DEV, :] = total.astype(out.dtype)
    out[ROWS_DEV:ROWS_DEV + EXTRA, :] = live_rows(live, out)


def last_kernel(tokens_all, *refs):
    total, live = gathered(refs[:-1])
    refs[-1][...] = total * (tokens_all / live)


def vmem(n):
    return [pl.BlockSpec(memory_space=pltpu.VMEM)] * n


def call(kernel, shapes, flops, *args):
    return pl.pallas_call(
        kernel,
        in_specs=vmem(len(args)),
        out_specs=vmem(len(shapes)) if isinstance(shapes, list) else vmem(1)[0],
        out_shape=shapes,
        compiler_params=pltpu.CompilerParams(vmem_limit_bytes=LIMIT),
        cost_estimate=pl.CostEstimate(flops=flops, bytes_accessed=1 << 20, transcendentals=0),
    )(*args)


def on_device(groups, batches, embeds, out_grad, w_query, w_key, w_value, lengths, item_rows,
              tile_owner):
    tokens, width = embeds.shape
    halves = 2
    tile = tokens // tile_owner.shape[0]
    owned = tile_owner.shape[0] // halves // groups
    pairs = batches // 2
    rows = item_rows.reshape(-1, tile)
    f32, bf16 = jnp.float32, jnp.bfloat16
    shape = jax.ShapeDtypeStruct
    far = groups - 1
    work = 2 * pairs * ROWS_DEV * width * owned * tile

    def swap(box, k):
        return lax.ppermute(box, "group", [(i, i ^ k) for i in range(groups)])

    def across(box, k):
        return lax.ppermute(box, "batch", [(i, i ^ k) for i in range(batches)])

    near = []
    mine = attention(
        0, halves, groups, lengths, tile_owner, embeds, out_grad, w_query, w_key, w_value, rows
    )
    w_all, (emb_next, gout_next) = mine[groups:groups + 3], mine[groups + 3:groups + 5]
    counts = mine[-1]
    for half in range(halves):
        if half:
            mine = attention(
                half, halves, groups, lengths, tile_owner, emb_next, gout_next, *w_all, counts, mine[far]
            )
        near.append([mine[0]] + [swap(mine[k], k) for k in range(far - 1, 0, -1)])
    away = mine[far]

    def parts_of(kernel, flops, *args):
        return call(
            kernel, [shape((ROWS_DEV + EXTRA, width), f32 if k == 0 else bf16) for k in range(pairs)],
            flops, *args,
        )

    far_parts = parts_of(
        functools.partial(far_pair_kernel, pairs, halves * owned, tile),
        4 * work, away, across(away, 1),
    )
    far_parts = [far_parts[0]] + [
        across(far_parts[k], 2 * k)
        for k in sorted(range(1, pairs), key=lambda k: (k == pairs // 2, -k))
    ]
    tall = pairs * ROWS_DEV
    send, own = [
        call(
            functools.partial(early_kernel, which, pairs, owned, tile, far),
            shape((rows_out, width), kind), (far + 1) * work, *near[0], near[1][0],
        )
        for which, rows_out, kind in ((0, tall + far * EXTRA, bf16), (1, tall, f32))
    ]
    got = across(send, 1)
    late = near[1][1:]
    near_parts = parts_of(
        functools.partial(near_pair_kernel, pairs, owned, tile, far),
        4 * work, *near[0], own, got, *late,
        *[across(box, 1) for box in late],
    )
    near_parts = [near_parts[0]] + [across(near_parts[k], 2 * k) for k in range(pairs - 1, 0, -1)]
    far_sum = call(far_kernel, shape((ROWS_DEV + EXTRA, width), bf16), 1 << 20, *far_parts)
    return call(
        functools.partial(last_kernel, float(tokens * groups * batches)),
        shape((ROWS_DEV, width), f32), 1 << 20, *near_parts, swap(far_sum, far),
    )


def solution(mesh):
    groups, batches = mesh.shape["group"], mesh.shape["batch"]
    both = P(("group", "batch"))
    wide = P(("group", "batch"), None)

    def body(*args):
        return on_device(groups, batches, *args)

    return jax.shard_map(
        body,
        mesh=mesh,
        in_specs=(wide, wide, P(), P(), P(), both, both, both),
        out_specs=wide,
        check_vma=False,
    )
```
